32 devices in a mesh: row: 4 (over z), col: 8 (over y, x, core).
Axes of the slice: x: 2, y: 2, z: 4, core: 2. Of those that a mesh axis runs over, the one named last changes fastest.
Arguments:
- node_latent: bfloat16 [32768, 128], P(('row', 'col')), may hold values from -6 to 6
- edge_latent: bfloat16 [131072, 128], P(('row', 'col')), may hold values from -6 to 6
- senders: int32 [131072], P(('row', 'col')), may hold values from 0 to 1535
- receivers: int32 [131072], P(('row', 'col')), may hold values from 0 to 1023
- send_index: int32 [32, 4, 128], P(('row', 'col')), may hold values from 0 to 1023
- context_table: bfloat16 [256, 128], P(('row', 'col')), may hold values from -6 to 6
- region: int32 [32768], P(('row', 'col')), may hold values from 0 to 255
- edge_w1: bfloat16 [2, 384, 128], replicated, may hold values from -0.3125 to 0.3125
- edge_w2: bfloat16 [2, 128, 128], replicated, may hold values from -0.5 to 0.5
- edge_bias: float32 [2, 3, 128], replicated, may hold values from -3 to 3
- edge_gain: float32 [2, 128], replicated, may hold values from 0.25 to 1.75
- node_w1: bfloat16 [2, 384, 128], replicated, may hold values from -0.3125 to 0.3125
- node_wg: bfloat16 [2, 128, 128], replicated, may hold values from -0.5 to 0.5
- node_w2: bfloat16 [2, 128, 128], replicated, may hold values from -0.5 to 0.5
- node_bias: float32 [2, 3, 128], replicated, may hold values from -3 to 3
- node_gain: float32 [2, 128], replicated, may hold values from 0.25 to 1.75
Outputs:
- node_out: bfloat16 [32768, 128], P(('row', 'col'))
- edge_out: bfloat16 [131072, 128], P(('row', 'col'))
The draws below stay inside these ranges and needn't reach their ends.
Inputs may be any that keep to these rules, and one draw needn't show every extreme that they name: senders index the extended table of the edge's own partition: below 1024 its own nodes, then the four received blocks of 128 rows in the order above, below, left, right. receivers are nodes of the edge's own partition. `send_index`: rows of the sending partition's own nodes; repeats may occur.
All inputs are finite; a program needn't handle non-finite values.
Results may differ from the reference program's by a relative error of at most 0.0085.
Values may be sent and summed in bfloat16 or wider, within the bound.
A program may use at most 64 MiB of HBM per device.

```python
import math
import jax
import jax.numpy as jnp
from jax import lax

LATENT = 128
NODES_DEV = 1024
BOUNDARY = 128
LAYERS = 2
EDGES_DEV = 4096
EXTENDED = 1536
PARTS_SIZE = 32
NODES = 32768
EDGES = 131072
REGIONS = 256
N_ROW = 4
N_COL = 8


def with_ends(values, key, low, high):
    shape = values.shape
    index_at = [jax.random.randint(jax.random.fold_in(key, axis), (), 0, shape[axis]) for axis in range(len(shape))]
    values = values.at[tuple(index_at)].set(low)
    longest = shape.index(max(shape))
    index_at[longest] = (index_at[longest] + 1) % shape[longest]
    return values.at[tuple(index_at)].set(high)


def steps_of(stream_key, extent, cuts, least, top_value):
    factor_of = 1.0
    for position, shards_of in cuts:
        steps = jax.random.uniform(jax.random.fold_in(jax.random.fold_in(stream_key, 6), position), (shards_of,), jnp.float32, least / len(cuts), top_value / len(cuts))
        factor_of = factor_of * jnp.repeat(jnp.exp(steps), extent[position] // shards_of).reshape((-1,) + (1,) * (len(extent) - 1 - position))
    return factor_of


def bell_draw(stream_key, dims, deviation, reach, cuts=(), dtype=jnp.bfloat16):
    level = steps_of(stream_key, dims, cuts, -0.22, 0.18) if cuts else 1.0
    drawn = jax.random.normal(stream_key, dims, jnp.float32) * deviation * level
    return jnp.minimum(jnp.maximum(drawn, -reach), reach).astype(dtype)


def setup_inputs(seed: int = 0) -> dict:
    splits = jax.random.split(jax.random.key(seed), 17)
    node_latent = bell_draw(splits[0], (NODES, LATENT), 1.0, 6.0, ((0, 32),))
    edge_latent = bell_draw(splits[1], (EDGES, LATENT), 1.0, 6.0, ((0, 32),))
    senders = with_ends(jax.random.randint(splits[2], (EDGES,), 0, EXTENDED), jax.random.fold_in(splits[2], 1), 0, EXTENDED - 1).astype(jnp.int32)
    receivers = with_ends(jax.random.randint(splits[3], (EDGES,), 0, NODES_DEV), jax.random.fold_in(splits[3], 1), 0, NODES_DEV - 1).astype(jnp.int32)
    send_index = with_ends(jax.random.randint(splits[4], (PARTS_SIZE, 4, BOUNDARY), 0, NODES_DEV), jax.random.fold_in(splits[4], 1), 0, NODES_DEV - 1).astype(jnp.int32)
    context_table = bell_draw(splits[5], (REGIONS, LATENT), 1.0, 6.0, ((0, 32),))
    region = with_ends(jax.random.randint(splits[6], (NODES,), 0, REGIONS), jax.random.fold_in(splits[6], 1), 0, REGIONS - 1).astype(jnp.int32)
    edge_w1 = bell_draw(splits[7], (LAYERS, 3 * LATENT, LATENT), (3 * LATENT) ** -0.5, 0.3125)
    edge_w2 = bell_draw(splits[8], (LAYERS, LATENT, LATENT), LATENT ** -0.5, 0.5)
    edge_bias = bell_draw(splits[9], (LAYERS, 3, LATENT), 0.5, 3.0, (), jnp.float32)
    edge_gain = jnp.clip(1.0 + 0.15 * jax.random.normal(splits[10], (LAYERS, LATENT), jnp.float32), 0.25, 1.75)
    node_w1 = bell_draw(splits[11], (LAYERS, 3 * LATENT, LATENT), (3 * LATENT) ** -0.5, 0.3125)
    node_wg = bell_draw(splits[12], (LAYERS, LATENT, LATENT), LATENT ** -0.5, 0.5)
    node_w2 = bell_draw(splits[13], (LAYERS, LATENT, LATENT), LATENT ** -0.5, 0.5)
    node_bias = bell_draw(splits[14], (LAYERS, 3, LATENT), 0.5, 3.0, (), jnp.float32)
    node_gain = jnp.clip(1.0 + 0.15 * jax.random.normal(splits[15], (LAYERS, LATENT), jnp.float32), 0.25, 1.75)
    return dict(node_latent=node_latent, edge_latent=edge_latent, senders=senders, receivers=receivers, send_index=send_index, context_table=context_table, region=region, edge_w1=edge_w1, edge_w2=edge_w2, edge_bias=edge_bias, edge_gain=edge_gain, node_w1=node_w1, node_wg=node_wg, node_w2=node_w2, node_bias=node_bias, node_gain=node_gain)


EPS = 1e-05

def norm_tail(pre, w_out, b_out, gain, shift):
    hidden = jax.nn.relu(pre).astype(jnp.bfloat16)
    y_val = jnp.dot(hidden, w_out, preferred_element_type=jnp.float32) + b_out
    centred = y_val - lax.optimization_barrier(jnp.mean(y_val, axis=-1, keepdims=True))
    spread = lax.optimization_barrier(jnp.mean(centred * centred, axis=-1, keepdims=True))
    return centred * lax.rsqrt(spread + EPS) * gain + shift

def edge_step(extended, edges, senders, receivers, w_in, w_out, bias, gain):
    feats = jnp.concatenate([jnp.take(extended, senders, axis=0), jnp.take(extended, receivers, axis=0), edges], axis=1)
    pre = jnp.dot(feats, w_in, preferred_element_type=jnp.float32) + bias[0]
    return (edges.astype(jnp.float32) + norm_tail(pre, w_out, bias[1], gain, bias[2])).astype(jnp.bfloat16)

def node_step(nodes, new_edges, receivers, context_rows, w_in, w_out, bias, gain, shift_in):
    summed = jax.ops.segment_sum(new_edges.astype(jnp.float32), receivers, num_segments=nodes.shape[0]).astype(jnp.bfloat16)
    feats = jnp.concatenate([nodes, summed, context_rows], axis=1)
    pre = jnp.dot(feats, w_in, preferred_element_type=jnp.float32) + shift_in
    return (nodes.astype(jnp.float32) + norm_tail(pre, w_out, bias[1], gain, bias[2])).astype(jnp.bfloat16)

def pick_rows(nodes, index):
    width = nodes.shape[1]
    return jnp.take(nodes, index.reshape(-1), axis=0).reshape(4, index.shape[1], width)

def with_halo(nodes, send_index):
    sent = jax.vmap(jax.vmap(pick_rows))(nodes, send_index)
    zero_row = jnp.zeros_like(sent[:1, :, 0])
    from_above = jnp.concatenate([zero_row, sent[:-1, :, 0]], axis=0)
    from_below = jnp.concatenate([sent[1:, :, 1], zero_row], axis=0)
    zero_col = jnp.zeros_like(sent[:, :1, 2])
    from_left = jnp.concatenate([zero_col, sent[:, :-1, 2]], axis=1)
    from_right = jnp.concatenate([sent[:, 1:, 3], zero_col], axis=1)
    return jnp.concatenate([nodes, from_above, from_below, from_left, from_right], axis=2)

def reference(node_latent, edge_latent, senders, receivers, send_index, context_table, region, edge_w1, edge_w2, edge_bias, edge_gain, node_w1, node_wg, node_w2, node_bias, node_gain):
    width = node_latent.shape[1]
    pooled = lax.optimization_barrier(jnp.sum(node_latent.astype(jnp.float32), axis=0)) / math.sqrt(NODES)
    nodes = node_latent.reshape(N_ROW, N_COL, NODES_DEV, width)
    edges = edge_latent.reshape(PARTS_SIZE, EDGES_DEV, width)
    sender_rows = senders.reshape(PARTS_SIZE, EDGES_DEV)
    receiver_rows = receivers.reshape(PARTS_SIZE, EDGES_DEV)
    index = send_index.reshape(N_ROW, N_COL, 4, BOUNDARY)
    context_rows = jnp.take(context_table, region, axis=0).reshape(PARTS_SIZE, NODES_DEV, width)
    for layer in range(LAYERS):
        extended = with_halo(nodes, index).reshape(PARTS_SIZE, EXTENDED, width)
        flat = nodes.reshape(PARTS_SIZE, NODES_DEV, width)
        shift_in = node_bias[layer, 0] + jnp.dot(pooled, node_wg[layer].astype(jnp.float32), precision=lax.Precision.HIGHEST)

        def one_part(items, layer=layer, shift_in=shift_in):
            ext_p, edges_p, send_p, recv_p, nodes_p, ctx_p = items
            new_edges = edge_step(ext_p, edges_p, send_p, recv_p, edge_w1[layer], edge_w2[layer], edge_bias[layer], edge_gain[layer])
            new_nodes = node_step(nodes_p, new_edges, recv_p, ctx_p, node_w1[layer], node_w2[layer], node_bias[layer], node_gain[layer], shift_in)
            return (new_edges, new_nodes)
        edges, flat = lax.map(one_part, (extended, edges, sender_rows, receiver_rows, flat, context_rows))
        nodes = flat.reshape(N_ROW, N_COL, NODES_DEV, width)
    return (nodes.reshape(NODES, width), edges.reshape(EDGES, width))
```

```python
import functools
import math

import jax
import jax.numpy as jnp
from jax import lax
from jax.experimental import pallas as pl
from jax.experimental.pallas import tpu as pltpu
from jax.sharding import PartitionSpec as P

LAYERS = 2
EPS = 1e-05
LANES = 128
BLOCK = 512
PAIR = 2 * BLOCK
F32 = jnp.float32
BF16 = jnp.bfloat16
I32 = jnp.int32
MESH = pl.DeviceIdType.MESH


def mm(a, b):
    return jnp.dot(a, b, preferred_element_type=F32)


def iota(axis):
    return lax.broadcasted_iota(I32, (LANES, LANES), axis)


def as_column(row):
    return jnp.transpose(jnp.broadcast_to(row, (LANES, LANES)))


def code(index):
    return (LANES + (index & (LANES - 1))) << (index >> 7)


def pick_parts(coded, axis, parts):
    base = (iota(axis) + LANES).astype(F32)
    one, zero = jnp.ones((), BF16), jnp.zeros((), BF16)
    return [
        jnp.where(coded == (base * float(1 << part)).astype(BF16), one, zero) for part in parts
    ]


def pick_rows(coded, parts):
    blocks = []
    for start in range(0, coded.shape[0], LANES):
        blocks.append(jnp.concatenate(pick_parts(coded[start : start + LANES], 1, parts), axis=1))
    return blocks[0] if len(blocks) == 1 else jnp.concatenate(blocks, axis=0)


def centre(values):
    values = values.astype(F32)
    return values - jnp.mean(values, axis=-1, keepdims=True)


def twice(weight):
    zero = jnp.zeros_like(weight)
    top = jnp.concatenate([weight, zero], axis=1)
    return jnp.concatenate([top, jnp.concatenate([zero, weight], axis=1)], axis=0)


def norm(centred, gain, shift):
    width = centred.shape[-1]
    total = jnp.sum(centred * centred, axis=-1, keepdims=True)
    return centred * lax.rsqrt(total + width * EPS) * (gain * math.sqrt(width)) + shift


def fold(ref):
    half = ref.shape[0] // 2
    return jnp.concatenate([ref[:half, :], ref[half:, :]], axis=1)


def kernel(
    n_row,
    n_col,
    early,
    rest,
    node_ref,
    edge_ref,
    send_ref,
    recv_ref,
    index_ref,
    ctx_ref,
    region_ref,
    ew1,
    ew2,
    eb,
    eg,
    nw1,
    nwg,
    nw2,
    nb,
    ng,
    node_out,
    edge_out,
    send_row,
    recv_row,
    send_code,
    recv_code,
    hot_sum,
    hot_index,
    hot_region,
    index_code,
    picked,
    halo,
    table,
    own_send,
    own_recv,
    halo_tab,
    pre_ref,
    sums,
    ctx_part,
    parts,
    edge_sem,
    halo_send_sem,
    halo_recv_sem,
    row_send_sem,
    row_recv_sem,
    col_send_sem,
    col_recv_sem,
    near_row_sem,
    near_col_sem,
    ready_row_sem,
    ready_col_sem,
):
    my_row, my_col = lax.axis_index("row"), lax.axis_index("col")
    devices = n_row * n_col
    nodes, width = node_ref.shape
    edges = edge_ref.shape[0]
    count = index_ref.shape[1]
    half_own, half_halo = nodes // 2, 2 * count
    own_parts = range(half_own // LANES)
    halo_parts = range(half_own // LANES, (half_own + half_halo) // LANES)
    ctx_rows = ctx_ref.shape[0]
    pairs = edges // PAIR

    def in_row(place):
        return (place, my_col)

    def in_col(place):
        return (my_row, place)

    def signal_all(sem, place, low, high):
        def one(other, carry):
            pl.semaphore_signal(sem, inc=1, device_id=place(other), device_id_type=MESH)
            return carry

        lax.fori_loop(low, high, one, 0)

    def wait_for(sem, value):
        @pl.when(value > 0)
        def _():
            pl.semaphore_wait(sem, value)

    edge_in = pltpu.make_async_copy(edge_ref, edge_out, edge_sem)
    edge_in.start()

    moves = (
        (my_row + 1, my_col, my_row < n_row - 1, my_row > 0),
        (my_row - 1, my_col, my_row > 0, my_row < n_row - 1),
        (my_row, my_col + 1, my_col < n_col - 1, my_col > 0),
        (my_row, my_col - 1, my_col > 0, my_col < n_col - 1),
    )
    barrier = pltpu.get_barrier_semaphore()
    signal_all(barrier, in_row, my_row + 1, n_row)
    signal_all(barrier, in_col, my_col + 1, n_col)

    with jax.named_scope("early"):
        for copy in early:
            copy.wait()

    def signed(index, upper):
        return code(index).astype(F32) * jnp.where(upper, -1.0, 1.0)

    sender, receiver = send_ref[...], recv_ref[...]
    in_halo = (sender >= nodes).astype(I32)
    part_size = half_own + (half_halo - half_own) * in_halo
    s_index = sender - nodes * in_halo
    s_upper = s_index >= part_size
    s_index += half_own * in_halo - part_size * s_upper.astype(I32)
    r_upper = receiver >= half_own
    send_row[...] = signed(s_index, s_upper)
    recv_row[...] = signed(receiver - half_own * r_upper.astype(I32), r_upper)

    for line in range(4):
        index = index_ref[line : line + 1, :]
        upper = index >= half_own
        column = as_column(signed(index - half_own * upper.astype(I32), upper))
        rows = slice(line * count, (line + 1) * count)
        index_code[rows, :] = column
        hot_index[rows, :] = pick_rows(jnp.abs(column.astype(BF16)), own_parts)

    def take(coded, both):
        return jnp.where(coded < 0, both[:, width:], both[:, :width])

    def pick(layer, now):
        picked[layer] = take(index_code[...], mm(hot_index[...], fold(now))).astype(BF16)

    pick(0, node_ref)
    part = jnp.sum(node_ref[...].astype(F32).reshape(nodes // 8, 8, width), axis=0)
    left = jnp.sum(part, axis=0, keepdims=True)
    pieces = []
    for _ in range(3):
        pieces.append(left.astype(BF16).astype(F32))
        left = left - pieces[-1]
    block = [ctx_ref[...].astype(F32)] + pieces + [jnp.zeros((5, width), F32)]
    table[my_col, my_row] = jnp.concatenate(block, axis=0).astype(BF16)

    def halo_copy(layer, line):
        rows = pl.ds(line * count, count)
        return pltpu.make_async_remote_copy(
            src_ref=picked.at[layer, rows],
            dst_ref=halo.at[layer, rows],
            send_sem=halo_send_sem.at[layer, line],
            recv_sem=halo_recv_sem.at[layer, line],
            device_id=moves[line][:2],
            device_id_type=MESH,
        )

    def halo_start(layer, lines):
        for line in lines:

            @pl.when(moves[line][2])
            def _(line=line):
                halo_copy(layer, line).start()

    def halo_wait(layer):
        for line in range(4):

            @pl.when(moves[line][3])
            def _(line=line):
                halo_copy(layer, line).wait_recv()

            @pl.when(jnp.logical_not(moves[line][3]))
            def _(line=line):
                halo[layer, line * count : (line + 1) * count] = jnp.zeros((count, width), BF16)

    def row_copy(other):
        return pltpu.make_async_remote_copy(
            src_ref=table.at[my_col, my_row],
            dst_ref=table.at[my_col, my_row],
            send_sem=row_send_sem,
            recv_sem=row_recv_sem,
            device_id=in_row(other),
            device_id_type=MESH,
        )

    def col_copy(other):
        return pltpu.make_async_remote_copy(
            src_ref=table.at[my_col],
            dst_ref=table.at[my_col],
            send_sem=col_send_sem,
            recv_sem=col_recv_sem,
            device_id=in_col(other),
            device_id_type=MESH,
        )

    def start_all(copy, low, high):
        def one(other, carry):
            copy(other).start()
            return carry

        lax.fori_loop(low, high, one, 0)

    def row_total():
        held = table.at[my_col, pl.ds(0, n_row - 1)]
        return pltpu.make_async_remote_copy(
            src_ref=held,
            dst_ref=held,
            send_sem=row_send_sem,
            recv_sem=row_recv_sem,
            device_id=in_row(lax.rem(my_row + 1, n_row)),
            device_id_type=MESH,
        )

    def col_total():
        held = table.at[pl.ds(0, n_col - 1)]
        return pltpu.make_async_remote_copy(
            src_ref=held,
            dst_ref=held,
            send_sem=col_send_sem,
            recv_sem=col_recv_sem,
            device_id=in_col(lax.rem(my_col + 1, n_col)),
            device_id_type=MESH,
        )

    with jax.named_scope("enter"):
        wait_for(barrier, my_row + my_col)

    @pl.when(my_row > 0)
    def _():
        pl.semaphore_signal(near_row_sem, inc=1, device_id=in_row(my_row - 1), device_id_type=MESH)

    @pl.when(my_col > 0)
    def _():
        pl.semaphore_signal(near_col_sem, inc=1, device_id=in_col(my_col - 1), device_id_type=MESH)

    halo_start(0, (1, 3))
    signal_all(ready_row_sem, in_row, 0, my_row)
    start_all(row_copy, 0, my_row)
    signal_all(ready_col_sem, in_col, 0, my_col)

    def near():
        wait_for(near_row_sem, moves[0][2].astype(I32))
        wait_for(near_col_sem, moves[2][2].astype(I32))
        halo_start(0, (0, 2))

    def first_phase():
        wait_for(ready_row_sem, n_row - 1 - my_row)
        start_all(row_copy, my_row + 1, n_row)

    def second_phase():
        row_total().wait_recv()
        wait_for(ready_col_sem, n_col - 1 - my_col)
        start_all(col_copy, 0, my_col)
        start_all(col_copy, my_col + 1, n_col)

    ahead = jnp.logical_and(my_row == 0, my_col < 2)
    near_pair = 1 + ahead.astype(I32)

    for copy in rest:
        copy.wait()
    edge_in.wait()

    def fill_own(layer, now):
        w_pair = jnp.concatenate([ew1[layer, :width], ew1[layer, width : 2 * width]], axis=1)
        both = mm(now[...], w_pair).astype(BF16)
        own_send[...] = jnp.concatenate([both[:half_own, :width], both[half_own:, :width]], axis=1)
        own_recv[...] = jnp.concatenate([both[:half_own, width:], both[half_own:, width:]], axis=1)

    def blocks_of(pair):
        return [
            pl.ds(pl.multiple_of(pair * PAIR + half * BLOCK, BLOCK), BLOCK) for half in range(2)
        ]

    def encode(pair):
        for sub in range(PAIR // LANES):
            line = pair * (PAIR // LANES) + sub
            rows = pl.ds(pl.multiple_of(line * LANES, LANES), LANES)
            recv = recv_row[pl.ds(line, 1), :]
            send_code[rows, :] = as_column(send_row[pl.ds(line, 1), :])
            recv_code[rows, :] = as_column(recv)
            across = jnp.broadcast_to(jnp.abs(recv), (LANES, LANES)).astype(BF16)
            for part, value in enumerate(pick_parts(across, 0, own_parts)):
                hot_sum[
                    pair, part * LANES : (part + 1) * LANES, sub * LANES : (sub + 1) * LANES
                ] = value

    def gather_phase(layer):
        w_edge = twice(ew1[layer, 2 * width :])
        b_in = eb[0, layer : layer + 1]

        def body(pair, carry):
            if layer == 0:

                @pl.when(pair == near_pair)
                def _():
                    near()

                @pl.when(jnp.logical_and(pair == pairs - 1, jnp.logical_not(ahead)))
                def _():
                    first_phase()

                encode(pair)
            blocks = blocks_of(pair)
            by_edge = mm(jnp.concatenate([edge_out[rows, :] for rows in blocks], axis=1), w_edge)
            for half, rows in enumerate(blocks):
                send, recv = send_code[rows, :], recv_code[rows, :]
                by_send = mm(pick_rows(jnp.abs(send.astype(BF16)), own_parts), own_send[...])
                by_recv = mm(pick_rows(jnp.abs(recv.astype(BF16)), own_parts), own_recv[...])
                pre = by_edge[:, half * width : (half + 1) * width] + b_in
                pre += take(send, by_send)
                pre += take(recv, by_recv)
                pre_ref[rows, :] = pre
            return carry

        lax.fori_loop(0, pairs, body, 0)

    def fill_halo(layer):
        rows = mm(halo[layer], ew1[layer, :width]).astype(BF16)
        halo_tab[...] = jnp.concatenate([rows[:half_halo], rows[half_halo:]], axis=1)

    def scatter(pair):
        term = mm(hot_sum[pair], parts[...])
        if pair == 0:
            sums[...] = term
        else:
            sums[...] += term

    def edge_phase(layer, first, last):
        w_out = twice(centre(ew2[layer]).astype(BF16))
        b_out = centre(eb[1, layer : layer + 1])
        for pair in range(first, last):
            starts = [pair * PAIR + half * BLOCK for half in range(2)]
            blocks = [slice(start, start + BLOCK) for start in starts]
            by_halo = [
                mm(pick_rows(jnp.abs(send_code[rows, :].astype(BF16)), halo_parts), halo_tab[...])
                for rows in blocks
            ]
            if pair > 0:
                scatter(pair - 1)
            hidden = []
            for half, rows in enumerate(blocks):
                pre = pre_ref[rows, :] + take(send_code[rows, :], by_halo[half])
                hidden.append(jnp.maximum(pre, 0.0).astype(BF16))
            y_val = mm(jnp.concatenate(hidden, axis=1), w_out)
            for half, rows in enumerate(blocks):
                centred = y_val[:, half * width : (half + 1) * width] + b_out
                new = edge_out[rows, :].astype(F32)
                new += norm(centred, eg[layer : layer + 1], eb[2, layer : layer + 1])
                new = new.astype(BF16)
                edge_out[rows, :] = new
                upper = recv_code[rows, :].astype(BF16) < 0
                held = slice(half * BLOCK, (half + 1) * BLOCK)
                zero = jnp.zeros((), BF16)
                parts[held, :width] = jnp.where(upper, zero, new)
                parts[held, width:] = jnp.where(upper, new, zero)

    def node_phase(layer, now):
        scatter(pairs - 1)
        summed = jnp.concatenate([sums[:, :width], sums[:, width:]], axis=0).astype(BF16)
        feats = jnp.concatenate([now[...], summed], axis=1)
        pre = mm(feats, nw1[layer, : 2 * width])
        pre += ctx_part[:, layer * width : (layer + 1) * width]
        hidden = jnp.maximum(pre, 0.0).astype(BF16)
        centred = mm(hidden, centre(nw2[layer]).astype(BF16)) + centre(nb[1, layer : layer + 1])
        new = now[...].astype(F32)
        new += norm(centred, ng[layer : layer + 1], nb[2, layer : layer + 1])
        node_out[...] = new.astype(BF16)

    def context():
        pieces = jnp.sum(table[:, :, ctx_rows:, :].astype(F32), axis=(0, 1))
        pooled = jnp.sum(pieces, axis=0, keepdims=True) / math.sqrt(nodes * devices)
        pieces = []
        for _ in range(3):
            pieces.append(pooled.astype(BF16).astype(F32))
            pooled = pooled - pieces[-1]
        pieces = jnp.concatenate(pieces + [jnp.zeros((13, width), F32)], axis=0).astype(BF16)
        w_global = jnp.concatenate([nwg[l] for l in range(LAYERS)], axis=1)
        shift = jnp.sum(mm(pieces, w_global), axis=0, keepdims=True)
        shift += jnp.concatenate([nb[0, l : l + 1] for l in range(LAYERS)], axis=1)
        shared = jnp.concatenate(
            [table[col, row, :ctx_rows] for row in range(n_row) for col in range(n_col)], axis=0
        )
        w_pair = jnp.concatenate([nw1[l, 2 * width :] for l in range(LAYERS)], axis=1)
        projected = mm(shared, w_pair).astype(BF16)
        ctx_part[...] = mm(hot_region[...], projected) + shift

    fill_own(0, node_ref)
    with jax.named_scope("gather0"):
        gather_phase(0)
    for line in range(nodes // LANES):
        column = as_column(code(region_ref[line : line + 1, :]).astype(F32))
        hot_region[line * LANES : (line + 1) * LANES, :] = pick_rows(
            column.astype(BF16), range(devices * ctx_rows // LANES)
        )
    with jax.named_scope("halo0"):
        halo_wait(0)
    fill_halo(0)
    edge_phase(0, 0, 1)

    @pl.when(ahead)
    def _():
        first_phase()

    @pl.when(jnp.logical_not(ahead))
    def _():
        second_phase()

    edge_phase(0, 1, 2)

    @pl.when(ahead)
    def _():
        second_phase()

    edge_phase(0, 2, pairs)
    with jax.named_scope("colwait"):
        col_total().wait_recv()
    context()
    node_phase(0, node_ref)
    pick(1, node_out)
    halo_start(1, range(4))
    fill_own(1, node_out)
    with jax.named_scope("gather1"):
        gather_phase(1)
    with jax.named_scope("halo1"):
        halo_wait(1)
    fill_halo(1)
    edge_phase(1, 0, pairs)
    node_phase(1, node_out)

    with jax.named_scope("sends"):
        for layer in range(LAYERS):
            for line in range(4):

                @pl.when(moves[line][2])
                def _(layer=layer, line=line):
                    halo_copy(layer, line).wait_send()

        row_total().wait_send()
        col_total().wait_send()


EARLY = (2, 3, 4, 0, 5)


def entry(n_row, n_col, count, *refs):
    given, others = refs[:count], list(refs[count : -count])
    held, copy_sem = refs[-count:-1], refs[-1]
    places = list(held)
    places.insert(1, None)
    copies = {
        k: pltpu.make_async_copy(given[k], places[k], copy_sem.at[k])
        for k in range(count)
        if k != 1
    }
    order = EARLY + tuple(k for k in copies if k not in EARLY)
    for k in order:
        copies[k].start()
    places[1] = given[1]
    early = [copies[k] for k in EARLY]
    rest = [copies[k] for k in order if k not in EARLY]
    kernel(n_row, n_col, early, rest, *places, *others)


def local(n_row, n_col, *args):
    node, edge, send, recv, index, ctx, region = args[:7]
    nodes, width = node.shape
    edges = edge.shape[0]
    count = index.shape[2]
    devices = n_row * n_col
    half_own, half_halo = nodes // 2, 2 * count
    vmem = pl.BlockSpec(memory_space=pltpu.VMEM)
    dma = pltpu.SemaphoreType.DMA
    operands = (
        node,
        edge,
        send.reshape(edges // LANES, LANES),
        recv.reshape(edges // LANES, LANES),
        index.reshape(4, count),
        ctx,
        region.reshape(nodes // LANES, LANES),
    ) + args[7:]
    operands = tuple(
        jnp.transpose(x, (1, 0, 2)) if x.shape == (LAYERS, 3, width) else x for x in operands
    )
    operands = tuple(pltpu.with_memory_space_constraint(x, pltpu.HBM) for x in operands)
    return pl.pallas_call(
        functools.partial(entry, n_row, n_col, len(operands)),
        out_shape=(
            jax.ShapeDtypeStruct(node.shape, BF16),
            jax.ShapeDtypeStruct(edge.shape, BF16),
        ),
        in_specs=[pl.BlockSpec(memory_space=pltpu.HBM)] * len(operands),
        out_specs=(vmem, vmem),
        scratch_shapes=[
            pltpu.VMEM((edges // LANES, LANES), F32),
            pltpu.VMEM((edges // LANES, LANES), F32),
            pltpu.VMEM((edges, width), F32),
            pltpu.VMEM((edges, width), F32),
            pltpu.VMEM((edges // PAIR, half_own, PAIR), BF16),
            pltpu.VMEM((4 * count, half_own), BF16),
            pltpu.VMEM((nodes, devices * ctx.shape[0]), BF16),
            pltpu.VMEM((4 * count, width), F32),
            pltpu.VMEM((LAYERS, 4 * count, width), BF16),
            pltpu.VMEM((LAYERS, 4 * count, width), BF16),
            pltpu.VMEM((n_col, n_row, ctx.shape[0] + 8, width), BF16),
            pltpu.VMEM((half_own, 2 * width), BF16),
            pltpu.VMEM((half_own, 2 * width), BF16),
            pltpu.VMEM((half_halo, 2 * width), BF16),
            pltpu.VMEM((edges, width), F32),
            pltpu.VMEM((half_own, 2 * width), F32),
            pltpu.VMEM((nodes, LAYERS * width), F32),
            pltpu.VMEM((PAIR, 2 * width), BF16),
            dma(()),
            dma((LAYERS, 4)),
            dma((LAYERS, 4)),
            dma(()),
            dma(()),
            dma(()),
            dma(()),
            pltpu.SemaphoreType.REGULAR,
            pltpu.SemaphoreType.REGULAR,
            pltpu.SemaphoreType.REGULAR,
            pltpu.SemaphoreType.REGULAR,
        ]
        + [pltpu.VMEM(x.shape, x.dtype) for k, x in enumerate(operands) if k != 1]
        + [dma((len(operands),))],
        compiler_params=pltpu.CompilerParams(
            collective_id=0, has_side_effects=True, vmem_limit_bytes=36 * 1024 * 1024
        ),
        name="mesh_steps",
    )(*operands)


def solution(mesh):
    both = ("row", "col")
    split = (P(both, None), P(both, None), P(both), P(both), P(both, None, None), P(both, None), P(both))
    return jax.shard_map(
        functools.partial(local, mesh.shape["row"], mesh.shape["col"]),
        mesh=mesh,
        in_specs=split + (P(),) * 9,
        out_specs=(P(both, None), P(both, None)),
        check_vma=False,
    )
```

```python
import functools
import math
import types

import jax
import jax.numpy as jnp
from jax import lax
from jax.experimental import pallas as pl
from jax.experimental.pallas import tpu as pltpu
from jax.sharding import PartitionSpec as P

LAYERS = 2
EPS = 1e-05
LANES = 128
BLOCK = 512
PAIR = 2 * BLOCK
F32 = jnp.float32
BF16 = jnp.bfloat16
I32 = jnp.int32
MESH = pl.DeviceIdType.MESH


def mm(a, b):
    return jnp.dot(a, b, preferred_element_type=F32)


def mm_halves(a, b):
    half = a.shape[0] // 2
    return jnp.concatenate([mm(a[:half], b), mm(a[half:], b)], axis=0)


def iota(axis):
    return lax.broadcasted_iota(I32, (LANES, LANES), axis)


def as_column(row):
    return jnp.transpose(jnp.broadcast_to(row, (LANES, LANES)))


def code(index):
    return (LANES + (index & (LANES - 1))) << (index >> 7)


def pick_parts(coded, axis, parts):
    base = (iota(axis) + LANES).astype(F32)
    one, zero = jnp.ones((), BF16), jnp.zeros((), BF16)
    if axis == 0:
        base = base.astype(BF16)
        masks = [coded * jnp.asarray(0.5**part, BF16) == base for part in parts]
    else:
        masks = [coded == (base * float(1 << part)).astype(BF16) for part in parts]
    return [jnp.where(mask, one, zero) for mask in masks]


def pick_rows(coded, parts):
    blocks = []
    for start in range(0, coded.shape[0], LANES):
        blocks.append(jnp.concatenate(pick_parts(coded[start : start + LANES], 1, parts), axis=1))
    return blocks[0] if len(blocks) == 1 else jnp.concatenate(blocks, axis=0)


def centre(values):
    values = values.astype(F32)
    return values - jnp.mean(values, axis=-1, keepdims=True)


def twice(weight):
    zero = jnp.zeros_like(weight)
    top = jnp.concatenate([weight, zero], axis=1)
    return jnp.concatenate([top, jnp.concatenate([zero, weight], axis=1)], axis=0)


def norm(centred, gain, shift):
    width = centred.shape[-1]
    total = jnp.sum(centred * centred, axis=-1, keepdims=True)
    return centred * lax.rsqrt(total + width * EPS) * (gain * math.sqrt(width)) + shift


def fold(ref):
    half = ref.shape[0] // 2
    return jnp.concatenate([ref[:half, :], ref[half:, :]], axis=1)


def take(coded, both):
    width = both.shape[1] // 2
    return jnp.where(coded < 0, both[:, width:], both[:, :width])


def scatter(at, pair):
    own_parts = range(at.sums.shape[0] // LANES)
    blocks = []
    for line in range(pair * PAIR // LANES, (pair + 1) * PAIR // LANES):
        coded = jnp.broadcast_to(jnp.abs(at.recv_row[line : line + 1, :]), (LANES, LANES))
        blocks.append(jnp.concatenate(pick_parts(coded.astype(BF16), 0, own_parts), axis=0))
    term = mm_halves(jnp.concatenate(blocks, axis=1), at.parts[pair % 2])
    if pair == 0:
        at.sums[...] = term
    else:
        at.sums[...] += term


def edge_phase(at, layer, old_ref, new_ref, ew1=None, done=None):
    edges, width = old_ref.shape
    half_own, half_halo = at.sums.shape[0], at.halo_tab.shape[0]
    pairs = edges // PAIR
    halo_parts = range(half_own // LANES, (half_own + half_halo) // LANES)
    w_out = twice(centre(at.ew2[layer]).astype(BF16))
    b_out = centre(at.eb[1, layer : layer + 1])
    if ew1 is not None:
        w_next = twice(ew1[layer + 1, 2 * width :])

    def blocks_of(pair):
        starts = [pair * PAIR + half * BLOCK for half in range(2)]
        return [slice(start, start + BLOCK) for start in starts]

    def columns(half):
        return slice(half * width, (half + 1) * width)

    def begin(pair):
        hidden = []
        for rows in blocks_of(pair):
            send = at.send_code[rows, :]
            hot = pick_rows(jnp.abs(send.astype(BF16)), halo_parts)
            pre = at.pre_ref[rows, :] + take(send, mm(hot, at.halo_tab[...]))
            hidden.append(jnp.maximum(pre.astype(BF16), jnp.zeros((), BF16)))
        at.y_ref[pair % 2] = mm_halves(jnp.concatenate(hidden, axis=1), w_out)

    def finish(pair):
        for half, rows in enumerate(blocks_of(pair)):
            centred = at.y_ref[pair % 2, :, columns(half)] + b_out
            new = old_ref[rows, :].astype(F32)
            new += norm(centred, at.eg[layer : layer + 1], at.eb[2, layer : layer + 1])
            new = new.astype(BF16)
            new_ref[rows, :] = new
            upper = at.recv_code[rows, :].astype(BF16) < 0
            held = slice(half * BLOCK, (half + 1) * BLOCK)
            zero = jnp.zeros((), BF16)
            at.parts[pair % 2, held, :width] = jnp.where(upper, zero, new)
            at.parts[pair % 2, held, width:] = jnp.where(upper, new, zero)

    def carry_on(pair):
        if ew1 is not None:
            news = [new_ref[rows, :] for rows in blocks_of(pair)]
            by_edge = mm(jnp.concatenate(news, axis=1), w_next)
            for half, rows in enumerate(blocks_of(pair)):
                at.pre_ref[rows, :] = by_edge[:, columns(half)] + at.eb[0, layer + 1 : layer + 2]

    for step in range(pairs + 1):
        if step < pairs:
            begin(step)
        if step > 1:
            scatter(at, step - 2)
            carry_on(step - 2)
        if step > 0:
            finish(step - 1)
        if done is not None and step > 1:
            done(step - 2)
    carry_on(pairs - 1)


def node_begin(at, layer, now):
    width = now.shape[1]
    scatter(at, at.recv_row.shape[0] * LANES // PAIR - 1)
    summed = jnp.concatenate([at.sums[:, :width], at.sums[:, width:]], axis=0).astype(BF16)
    feats = jnp.concatenate([now[...], summed], axis=1)
    return mm_halves(feats, at.nw1[layer, : 2 * width])


def node_end(at, layer, now, pre, new_ref):
    width = now.shape[1]
    pre += at.ctx_part[:, layer * width : (layer + 1) * width]
    hidden = jnp.maximum(pre, 0.0).astype(BF16)
    w_out, b_out = centre(at.nw2[layer]).astype(BF16), centre(at.nb[1, layer : layer + 1])
    new = now[...].astype(F32)
    new += norm(mm_halves(hidden, w_out) + b_out, at.ng[layer : layer + 1], at.nb[2, layer : layer + 1])
    new_ref[...] = new.astype(BF16)


def first_kernel(
    n_row,
    n_col,
    early,
    later,
    rest,
    node_ref,
    edge_ref,
    send_ref,
    recv_ref,
    index_ref,
    ctx_ref,
    region_ref,
    ew1,
    nwg,
    edge_sem,
    at,
    node_out,
    edge_out,
    send_row,
    hot_index,
    hot_region,
    index_code,
    picked,
    halo,
    table,
    pool,
    node_pre,
    own_send,
    own_recv,
    halo_send_sem,
    halo_recv_sem,
    row_send_sem,
    row_recv_sem,
    col_send_sem,
    col_recv_sem,
    near_row_sem,
    near_col_sem,
    ready_row_sem,
    ready_col_sem,
):
    my_row, my_col = lax.axis_index("row"), lax.axis_index("col")
    send_code, recv_code, recv_row = at.send_code, at.recv_code, at.recv_row
    halo_tab, pre_ref, ctx_part = at.halo_tab, at.pre_ref, at.ctx_part
    eb, nw1, nb = at.eb, at.nw1, at.nb
    devices = n_row * n_col
    nodes, width = node_ref.shape
    edges = edge_ref.shape[0]
    count = index_ref.shape[1]
    half_own, half_halo = nodes // 2, 2 * count
    own_parts = range(half_own // LANES)
    ctx_rows = ctx_ref.shape[0]
    pairs = edges // PAIR

    def in_row(place):
        return (place, my_col)

    def in_col(place):
        return (my_row, place)

    def signal_all(sem, place, low, high):
        def one(other, carry):
            pl.semaphore_signal(sem, inc=1, device_id=place(other), device_id_type=MESH)
            return carry

        lax.fori_loop(low, high, one, 0)

    def wait_for(sem, value):
        @pl.when(value > 0)
        def _():
            pl.semaphore_wait(sem, value)

    edge_in = pltpu.make_async_copy(edge_ref, edge_out, edge_sem)
    edge_in.start()

    moves = (
        (my_row + 1, my_col, my_row < n_row - 1, my_row > 0),
        (my_row - 1, my_col, my_row > 0, my_row < n_row - 1),
        (my_row, my_col + 1, my_col < n_col - 1, my_col > 0),
        (my_row, my_col - 1, my_col > 0, my_col < n_col - 1),
    )
    barrier = pltpu.get_barrier_semaphore()
    signal_all(barrier, in_row, my_row + 1, n_row)
    signal_all(barrier, in_col, my_col + 1, n_col)

    with jax.named_scope("early"):
        for copy in early:
            copy.wait()

    part = jnp.sum(node_ref[...].astype(F32).reshape(nodes // 8, 8, width), axis=0)
    pool[my_col, my_row] = jnp.sum(part, axis=0, keepdims=True)
    table[my_col, my_row] = ctx_ref[...]

    def halo_copy(layer, line):
        rows = pl.ds(line * count, count)
        return pltpu.make_async_remote_copy(
            src_ref=picked.at[layer, rows],
            dst_ref=halo.at[layer, rows],
            send_sem=halo_send_sem.at[layer, line],
            recv_sem=halo_recv_sem.at[layer, line],
            device_id=moves[line][:2],
            device_id_type=MESH,
        )

    def halo_start(layer, lines):
        for line in lines:

            @pl.when(moves[line][2])
            def _(line=line):
                halo_copy(layer, line).start()

    def halo_wait(layer):
        for line in range(4):

            @pl.when(moves[line][3])
            def _(line=line):
                halo_copy(layer, line).wait_recv()

            @pl.when(jnp.logical_not(moves[line][3]))
            def _(line=line):
                halo[layer, line * count : (line + 1) * count] = jnp.zeros((count, width), BF16)

    def row_copies(other):
        return [
            pltpu.make_async_remote_copy(
                src_ref=ref.at[my_col, my_row],
                dst_ref=ref.at[my_col, my_row],
                send_sem=row_send_sem.at[k],
                recv_sem=row_recv_sem.at[k],
                device_id=in_row(other),
                device_id_type=MESH,
            )
            for k, ref in enumerate((table, pool))
        ]

    def col_copies(other):
        return [
            pltpu.make_async_remote_copy(
                src_ref=ref.at[my_col],
                dst_ref=ref.at[my_col],
                send_sem=col_send_sem.at[k],
                recv_sem=col_recv_sem.at[k],
                device_id=in_col(other),
                device_id_type=MESH,
            )
            for k, ref in enumerate((table, pool))
        ]

    def start_all(copies, low, high):
        def one(other, carry):
            for copy in copies(other):
                copy.start()
            return carry

        lax.fori_loop(low, high, one, 0)

    def row_totals():
        held = [ref.at[my_col, pl.ds(0, n_row - 1)] for ref in (table, pool)]
        return [
            pltpu.make_async_remote_copy(
                src_ref=ref,
                dst_ref=ref,
                send_sem=row_send_sem.at[k],
                recv_sem=row_recv_sem.at[k],
                device_id=in_row(lax.rem(my_row + 1, n_row)),
                device_id_type=MESH,
            )
            for k, ref in enumerate(held)
        ]

    def col_totals():
        held = [ref.at[pl.ds(0, n_col - 1)] for ref in (table, pool)]
        return [
            pltpu.make_async_remote_copy(
                src_ref=ref,
                dst_ref=ref,
                send_sem=col_send_sem.at[k],
                recv_sem=col_recv_sem.at[k],
                device_id=in_col(lax.rem(my_col + 1, n_col)),
                device_id_type=MESH,
            )
            for k, ref in enumerate(held)
        ]

    row_known = jnp.minimum(my_row + 2, n_row)

    def near():
        wait_for(near_row_sem, moves[0][2].astype(I32))
        wait_for(near_col_sem, moves[2][2].astype(I32))
        halo_start(0, (0, 2))
        start_all(row_copies, my_row + 1, row_known)

    def first_phase():
        wait_for(ready_row_sem, n_row - 1 - my_row)
        start_all(row_copies, row_known, n_row)

    def second_phase():
        for copy in row_totals():
            copy.wait_recv()
        wait_for(ready_col_sem, n_col - 1 - my_col)
        start_all(col_copies, 0, my_col)
        start_all(col_copies, my_col + 1, n_col)

    ahead = jnp.logical_and(my_row == 0, my_col < 2)

    def between(pair, half):
        if (pair, half) == (1, 0):

            @pl.when(jnp.logical_not(ahead))
            def _():
                near()

        if (pair, half) == (2, 1):

            @pl.when(ahead)
            def _():
                near()

            @pl.when(jnp.logical_not(ahead))
            def _():
                first_phase()

    with jax.named_scope("enter"):
        wait_for(barrier, my_row + my_col)
    start_all(row_copies, 0, my_row)
    signal_all(ready_row_sem, in_row, 0, my_row)

    @pl.when(my_row > 0)
    def _():
        pl.semaphore_signal(near_row_sem, inc=1, device_id=in_row(my_row - 1), device_id_type=MESH)

    @pl.when(my_col > 0)
    def _():
        pl.semaphore_signal(near_col_sem, inc=1, device_id=in_col(my_col - 1), device_id_type=MESH)

    signal_all(ready_col_sem, in_col, 0, my_col)

    for copy in later:
        copy.wait()

    def signed(index, upper):
        return code(index).astype(F32) * jnp.where(upper, -1.0, 1.0)

    sender, receiver = send_ref[...], recv_ref[...]
    in_halo = (sender >= nodes).astype(I32)
    part_size = half_own + (half_halo - half_own) * in_halo
    s_index = sender - nodes * in_halo
    s_upper = s_index >= part_size
    s_index += half_own * in_halo - part_size * s_upper.astype(I32)
    r_upper = receiver >= half_own
    send_row[...] = signed(s_index, s_upper)
    recv_row[...] = signed(receiver - half_own * r_upper.astype(I32), r_upper)

    for line in range(4):
        index = index_ref[line : line + 1, :]
        upper = index >= half_own
        column = as_column(signed(index - half_own * upper.astype(I32), upper))
        rows = slice(line * count, (line + 1) * count)
        index_code[rows, :] = column
        hot_index[rows, :] = pick_rows(jnp.abs(column.astype(BF16)), own_parts)

    def pick(layer, now):
        picked[layer] = take(index_code[...], mm_halves(hot_index[...], fold(now))).astype(BF16)

    pick(0, node_ref)
    halo_start(0, (1, 3))
    with jax.named_scope("rest"):
        for copy in rest:
            copy.wait()
    edge_in.wait()

    def fill_own(layer, now):
        w_pair = jnp.concatenate([ew1[layer, :width], ew1[layer, width : 2 * width]], axis=1)
        both = mm_halves(now[...], w_pair).astype(BF16)
        own_send[...] = jnp.concatenate([both[:half_own, :width], both[half_own:, :width]], axis=1)
        own_recv[...] = jnp.concatenate([both[:half_own, width:], both[half_own:, width:]], axis=1)

    def encode(pair):
        for sub in range(PAIR // LANES):
            line = pair * (PAIR // LANES) + sub
            rows = slice(line * LANES, (line + 1) * LANES)
            recv = recv_row[line : line + 1, :]
            send_code[rows, :] = as_column(send_row[line : line + 1, :])
            recv_code[rows, :] = as_column(recv)

    def gather_phase(layer):
        if layer == 0:
            w_edge = twice(ew1[layer, 2 * width :])
            b_in = eb[0, layer : layer + 1]

        for pair in range(pairs):
            if layer == 0:
                between(pair, 0)
                encode(pair)
            starts = [pair * PAIR + half * BLOCK for half in range(2)]
            blocks = [slice(start, start + BLOCK) for start in starts]
            if layer == 0:
                old = [edge_out[rows, :] for rows in blocks]
                by_edge = mm(jnp.concatenate(old, axis=1), w_edge)
            for half, rows in enumerate(blocks):
                if layer == 0 and half == 1:
                    between(pair, 1)
                send, recv = send_code[rows, :], recv_code[rows, :]
                by_send = mm(pick_rows(jnp.abs(send.astype(BF16)), own_parts), own_send[...])
                by_recv = mm(pick_rows(jnp.abs(recv.astype(BF16)), own_parts), own_recv[...])
                if layer == 0:
                    pre = by_edge[:, half * width : (half + 1) * width] + b_in
                else:
                    pre = pre_ref[rows, :]
                pre += take(send, by_send)
                pre += take(recv, by_recv)
                pre_ref[rows, :] = pre

    def fill_halo(layer):
        rows = mm_halves(halo[layer], ew1[layer, :width]).astype(BF16)
        halo_tab[...] = jnp.concatenate([rows[:half_halo], rows[half_halo:]], axis=1)

    def context():
        pooled = jnp.zeros((1, width), F32)
        for col in range(n_col):
            for row in range(n_row):
                pooled += pool[col, row]
        pooled = pooled / math.sqrt(nodes * devices)
        pieces = []
        for _ in range(3):
            pieces.append(pooled.astype(BF16).astype(F32))
            pooled = pooled - pieces[-1]
        pieces = jnp.concatenate(pieces + [jnp.zeros((13, width), F32)], axis=0).astype(BF16)
        w_global = jnp.concatenate([nwg[l] for l in range(LAYERS)], axis=1)
        shift = jnp.sum(mm(pieces, w_global), axis=0, keepdims=True)
        shift += jnp.concatenate([nb[0, l : l + 1] for l in range(LAYERS)], axis=1)
        shared = jnp.concatenate(
            [table[col, row] for row in range(n_row) for col in range(n_col)], axis=0
        )
        w_pair = jnp.concatenate([nw1[l, 2 * width :] for l in range(LAYERS)], axis=1)
        projected = mm(shared, w_pair).astype(BF16)
        ctx_part[...] = mm_halves(hot_region[...], projected) + shift

    fill_own(0, node_ref)
    with jax.named_scope("gather0"):
        gather_phase(0)
    for line in range(nodes // LANES):
        column = as_column(code(region_ref[line : line + 1, :]).astype(F32))
        hot_region[line * LANES : (line + 1) * LANES, :] = pick_rows(
            column.astype(BF16), range(devices * ctx_rows // LANES)
        )
    @pl.when(ahead)
    def _():
        first_phase()

    with jax.named_scope("second"):
        second_phase()
    with jax.named_scope("halo0"):
        halo_wait(0)
    fill_halo(0)
    edge_phase(at, 0, edge_out, edge_out, ew1)
    node_pre[...] = node_begin(at, 0, node_ref)
    with jax.named_scope("colwait"):
        for copy in col_totals():
            copy.wait_recv()
    context()
    node_end(at, 0, node_ref, node_pre[...], node_out)
    pick(1, node_out)
    halo_start(1, range(4))
    fill_own(1, node_out)
    with jax.named_scope("gather1"):
        gather_phase(1)
    with jax.named_scope("halo1"):
        halo_wait(1)
    fill_halo(1)

    with jax.named_scope("sends"):
        for layer in range(LAYERS):
            for line in range(4):

                @pl.when(moves[line][2])
                def _(layer=layer, line=line):
                    halo_copy(layer, line).wait_send()

        for copy in row_totals() + col_totals():
            copy.wait_send()


HELD = ("ew2", "eb", "eg", "nw1", "nw2", "nb", "ng")
CARRIED = ("send_code", "recv_code", "recv_row", "halo_tab", "pre_ref", "ctx_part")


def first_entry(n_row, n_col, *refs):
    given, refs = refs[:16], refs[16:]
    outs, refs = refs[: 2 + len(CARRIED) + len(HELD)], refs[2 + len(CARRIED) + len(HELD) :]
    node_out, edge_out = outs[:2]
    at = types.SimpleNamespace(**dict(zip(CARRIED + HELD, outs[2:])))
    at.sums, at.parts, at.y_ref, edge_sem, copy_sem = refs[:5]
    node, send, recv, index, ctx, region, ew1, nwg = refs[5:13]
    places = [node, None, send, recv, index, ctx, region, ew1, at.ew2, at.eb, at.eg]
    places += [at.nw1, nwg, at.nw2, at.nb, at.ng]
    copies = {
        k: pltpu.make_async_copy(given[k], place, copy_sem.at[k])
        for k, place in enumerate(places)
        if place is not None
    }
    groups = (0, 5), (4, 2, 3)
    groups += (tuple(k for k in copies if k not in sum(groups, ())),)
    for k in sum(groups, ()):
        copies[k].start()
    groups = [[copies[k] for k in group] for group in groups]
    places[1] = given[1]
    first_kernel(n_row, n_col, *groups, *places[:8], nwg, edge_sem, at, node_out, edge_out, *refs[13:])


def second_entry(*refs):
    node, edge, refs = refs[0], refs[1], refs[2:]
    count = len(CARRIED) + len(HELD)
    at = types.SimpleNamespace(**dict(zip(CARRIED + HELD, refs[:count])))
    node_out, edge_out, node_new, edge_new, at.sums, at.parts, at.y_ref = refs[count : count + 7]
    node_sem, edge_sem = refs[count + 7 :]
    pairs = edge.shape[0] // PAIR

    def edge_copy(pair):
        rows = pl.ds(pair * PAIR, PAIR)
        return pltpu.make_async_copy(edge_new.at[rows], edge_out.at[rows], edge_sem.at[pair])

    edge_phase(at, 1, edge, edge_new, done=lambda pair: edge_copy(pair).start())
    edge_copy(pairs - 1).start()
    node_end(at, 1, node, node_begin(at, 1, node), node_new)
    node_copy = pltpu.make_async_copy(node_new, node_out, node_sem)
    node_copy.start()
    for pair in range(pairs):
        edge_copy(pair).wait()
    node_copy.wait()


def local(n_row, n_col, *args):
    node, edge, send, recv, index, ctx, region = args[:7]
    nodes, width = node.shape
    edges = edge.shape[0]
    count = index.shape[2]
    devices = n_row * n_col
    half_own, half_halo = nodes // 2, 2 * count
    vmem = pl.BlockSpec(memory_space=pltpu.VMEM)
    hbm = pl.BlockSpec(memory_space=pltpu.HBM)
    dma = pltpu.SemaphoreType.DMA
    operands = (
        node,
        edge,
        send.reshape(edges // LANES, LANES),
        recv.reshape(edges // LANES, LANES),
        index.reshape(4, count),
        ctx,
        region.reshape(nodes // LANES, LANES),
    ) + args[7:]
    operands = tuple(
        jnp.transpose(x, (1, 0, 2)) if x.shape == (LAYERS, 3, width) else x for x in operands
    )
    operands = tuple(pltpu.with_memory_space_constraint(x, pltpu.HBM) for x in operands)
    held = [operands[k] for k in (8, 9, 10, 11, 13, 14, 15)]
    carried = [
        ((edges, width), F32),
        ((edges, width), F32),
        ((edges // LANES, LANES), F32),
        ((half_halo, 2 * width), BF16),
        ((edges, width), F32),
        ((nodes, LAYERS * width), F32),
    ]
    shared = [
        jax.ShapeDtypeStruct(node.shape, BF16),
        jax.ShapeDtypeStruct(edge.shape, BF16),
    ]
    passed = shared + [jax.ShapeDtypeStruct(*x) for x in carried]
    passed += [jax.ShapeDtypeStruct(x.shape, x.dtype) for x in held]
    local_scratch = [
        pltpu.VMEM((half_own, 2 * width), F32),
        pltpu.VMEM((2, PAIR, 2 * width), BF16),
        pltpu.VMEM((2, BLOCK, 2 * width), F32),
    ]
    between = pl.pallas_call(
        functools.partial(first_entry, n_row, n_col),
        out_shape=tuple(passed),
        in_specs=[hbm] * len(operands),
        out_specs=(vmem,) * len(passed),
        scratch_shapes=local_scratch
        + [dma(()), dma((len(operands),))]
        + [pltpu.VMEM(operands[k].shape, operands[k].dtype) for k in (0, 2, 3, 4, 5, 6, 7, 12)]
        + [
            pltpu.VMEM((edges // LANES, LANES), F32),
            pltpu.VMEM((4 * count, half_own), BF16),
            pltpu.VMEM((nodes, devices * ctx.shape[0]), BF16),
            pltpu.VMEM((4 * count, width), F32),
            pltpu.VMEM((LAYERS, 4 * count, width), BF16),
            pltpu.VMEM((LAYERS, 4 * count, width), BF16),
            pltpu.VMEM((n_col, n_row, ctx.shape[0], width), BF16),
            pltpu.VMEM((n_col, n_row, 1, width), F32),
            pltpu.VMEM((nodes, width), F32),
            pltpu.VMEM((half_own, 2 * width), BF16),
            pltpu.VMEM((half_own, 2 * width), BF16),
            dma((LAYERS, 4)),
            dma((LAYERS, 4)),
            dma((2,)),
            dma((2,)),
            dma((2,)),
            dma((2,)),
            pltpu.SemaphoreType.REGULAR,
            pltpu.SemaphoreType.REGULAR,
            pltpu.SemaphoreType.REGULAR,
            pltpu.SemaphoreType.REGULAR,
        ],
        compiler_params=pltpu.CompilerParams(
            collective_id=0, has_side_effects=True, vmem_limit_bytes=24 * 1024 * 1024
        ),
        name="mesh_first",
    )(*operands)
    return pl.pallas_call(
        second_entry,
        out_shape=tuple(shared),
        in_specs=[vmem] * len(passed),
        out_specs=(hbm, hbm),
        scratch_shapes=[pltpu.VMEM(node.shape, BF16), pltpu.VMEM(edge.shape, BF16)]
        + local_scratch
        + [dma(()), dma((edges // PAIR,))],
        compiler_params=pltpu.CompilerParams(vmem_limit_bytes=24 * 1024 * 1024),
        name="mesh_second",
    )(*between)


def solution(mesh):
    both = ("row", "col")
    split = (P(both, None), P(both, None), P(both), P(both), P(both, None, None), P(both, None), P(both))
    return jax.shard_map(
        functools.partial(local, mesh.shape["row"], mesh.shape["col"]),
        mesh=mesh,
        in_specs=split + (P(),) * 9,
        out_specs=(P(both, None), P(both, None)),
        check_vma=False,
    )
```

```python
import functools
import math
import types

import jax
import jax.numpy as jnp
from jax import lax
from jax.experimental import pallas as pl
from jax.experimental.pallas import tpu as pltpu
from jax.sharding import PartitionSpec as P

LAYERS = 2
EPS = 1e-05
LANES = 128
BLOCK = 512
PAIR = 2 * BLOCK
F32 = jnp.float32
BF16 = jnp.bfloat16
I32 = jnp.int32
MESH = pl.DeviceIdType.MESH


def mm(a, b):
    return jnp.dot(a, b, preferred_element_type=F32)


def mm_halves(a, b):
    half = a.shape[0] // 2
    return jnp.concatenate([mm(a[:half], b), mm(a[half:], b)], axis=0)


def iota(axis):
    return lax.broadcasted_iota(I32, (LANES, LANES), axis)


def as_column(row):
    return jnp.transpose(jnp.broadcast_to(row, (LANES, LANES)))


def code(index):
    return (LANES + (index & (LANES - 1))) << (index >> 7)


def pick_parts(coded, axis, parts):
    base = (iota(axis) + LANES).astype(F32)
    one, zero = jnp.ones((), BF16), jnp.zeros((), BF16)
    if axis == 0:
        base = base.astype(BF16)
        masks = [coded * jnp.asarray(0.5**part, BF16) == base for part in parts]
    else:
        masks = [coded == (base * float(1 << part)).astype(BF16) for part in parts]
    return [jnp.where(mask, one, zero) for mask in masks]


def pick_rows(coded, parts):
    blocks = []
    for start in range(0, coded.shape[0], LANES):
        blocks.append(jnp.concatenate(pick_parts(coded[start : start + LANES], 1, parts), axis=1))
    return blocks[0] if len(blocks) == 1 else jnp.concatenate(blocks, axis=0)


def centre(values):
    values = values.astype(F32)
    return values - jnp.mean(values, axis=-1, keepdims=True)


def twice(weight):
    zero = jnp.zeros_like(weight)
    top = jnp.concatenate([weight, zero], axis=1)
    return jnp.concatenate([top, jnp.concatenate([zero, weight], axis=1)], axis=0)


def norm(centred, gain, shift):
    width = centred.shape[-1]
    total = jnp.sum(centred * centred, axis=-1, keepdims=True)
    return centred * lax.rsqrt(total + width * EPS) * (gain * math.sqrt(width)) + shift


def fold(ref):
    half = ref.shape[0] // 2
    return jnp.concatenate([ref[:half, :], ref[half:, :]], axis=1)


def take(coded, both):
    width = both.shape[1] // 2
    return jnp.where(coded < 0, both[:, width:], both[:, :width])


def scatter(at, pair):
    own_parts = range(at.sums.shape[0] // LANES)
    blocks = []
    for line in range(pair * PAIR // LANES, (pair + 1) * PAIR // LANES):
        coded = jnp.broadcast_to(jnp.abs(at.recv_row[line : line + 1, :]), (LANES, LANES))
        blocks.append(jnp.concatenate(pick_parts(coded.astype(BF16), 0, own_parts), axis=0))
    term = mm_halves(jnp.concatenate(blocks, axis=1), at.parts[...])
    if pair == 0:
        at.sums[...] = term
    else:
        at.sums[...] += term


def edge_phase(at, layer, old_ref, new_ref, ew1=None, done=None):
    edges, width = old_ref.shape
    half_own, half_halo = at.sums.shape[0], at.halo_tab.shape[0]
    pairs = edges // PAIR
    halo_parts = range(half_own // LANES, (half_own + half_halo) // LANES)
    w_out = twice(centre(at.ew2[layer]).astype(BF16))
    b_out = centre(at.eb[1, layer : layer + 1])
    if ew1 is not None:
        w_next = twice(ew1[layer + 1, 2 * width :])

    def blocks_of(pair):
        starts = [pair * PAIR + half * BLOCK for half in range(2)]
        return [slice(start, start + BLOCK) for start in starts]

    def columns(half):
        return slice(half * width, (half + 1) * width)

    def begin(pair):
        hidden = []
        for rows in blocks_of(pair):
            send = at.send_code[rows, :]
            hot = pick_rows(jnp.abs(send.astype(BF16)), halo_parts)
            pre = at.pre_ref[rows, :] + take(send, mm(hot, at.halo_tab[...]))
            hidden.append(jnp.maximum(pre.astype(BF16), jnp.zeros((), BF16)))
        at.y_ref[pair % 2] = mm_halves(jnp.concatenate(hidden, axis=1), w_out)

    def finish(pair):
        for half, rows in enumerate(blocks_of(pair)):
            centred = at.y_ref[pair % 2, :, columns(half)] + b_out
            new = old_ref[rows, :].astype(F32)
            new += norm(centred, at.eg[layer : layer + 1], at.eb[2, layer : layer + 1])
            new = new.astype(BF16)
            new_ref[rows, :] = new
            upper = at.recv_code[rows, :].astype(BF16) < 0
            held = slice(half * BLOCK, (half + 1) * BLOCK)
            zero = jnp.zeros((), BF16)
            at.parts[held, :width] = jnp.where(upper, zero, new)
            at.parts[held, width:] = jnp.where(upper, new, zero)

    def carry_on(pair):
        if ew1 is not None:
            news = [new_ref[rows, :] for rows in blocks_of(pair)]
            by_edge = mm(jnp.concatenate(news, axis=1), w_next)
            for half, rows in enumerate(blocks_of(pair)):
                at.pre_ref[rows, :] = by_edge[:, columns(half)] + at.eb[0, layer + 1 : layer + 2]

    for step in range(pairs + 1):
        if step < pairs:
            begin(step)
        if step > 1:
            scatter(at, step - 2)
            carry_on(step - 2)
        if step > 0:
            finish(step - 1)
        if done is not None and step > 1:
            done(step - 2)
    carry_on(pairs - 1)


def fill_halo(halo_tab, halo, weight):
    rows = mm_halves(halo, weight).astype(BF16)
    half = rows.shape[0] // 2
    halo_tab[...] = jnp.concatenate([rows[:half], rows[half:]], axis=1)


def node_begin(at, layer, now):
    width = now.shape[1]
    scatter(at, at.recv_row.shape[0] * LANES // PAIR - 1)
    summed = jnp.concatenate([at.sums[:, :width], at.sums[:, width:]], axis=0).astype(BF16)
    feats = jnp.concatenate([now[...], summed], axis=1)
    return mm_halves(feats, at.nw1[layer, : 2 * width])


def node_end(at, layer, now, pre, new_ref):
    width = now.shape[1]
    pre += at.ctx_part[:, layer * width : (layer + 1) * width]
    hidden = jnp.maximum(pre, 0.0).astype(BF16)
    w_out, b_out = centre(at.nw2[layer]).astype(BF16), centre(at.nb[1, layer : layer + 1])
    new = now[...].astype(F32)
    new += norm(mm_halves(hidden, w_out) + b_out, at.ng[layer : layer + 1], at.nb[2, layer : layer + 1])
    new_ref[...] = new.astype(BF16)


def first_kernel(
    n_row,
    n_col,
    early,
    later,
    rest,
    node_ref,
    edge_ref,
    send_ref,
    recv_ref,
    index_ref,
    ctx_ref,
    region_ref,
    ew1,
    nwg,
    edge_sem,
    at,
    node_out,
    edge_out,
    send_row,
    hot_index,
    hot_region,
    index_code,
    picked,
    halo,
    table,
    pool,
    node_pre,
    own_send,
    own_recv,
    halo_send_sem,
    halo_recv_sem,
    row_send_sem,
    row_recv_sem,
    col_send_sem,
    col_recv_sem,
    near_row_sem,
    near_col_sem,
    ready_row_sem,
    ready_col_sem,
):
    my_row, my_col = lax.axis_index("row"), lax.axis_index("col")
    send_code, recv_code, recv_row = at.send_code, at.recv_code, at.recv_row
    pre_ref, ctx_part = at.pre_ref, at.ctx_part
    eb, nw1, nb = at.eb, at.nw1, at.nb
    devices = n_row * n_col
    nodes, width = node_ref.shape
    edges = edge_ref.shape[0]
    count = index_ref.shape[1]
    half_own, half_halo = nodes // 2, 2 * count
    own_parts = range(half_own // LANES)
    ctx_rows = ctx_ref.shape[0]
    pairs = edges // PAIR

    def in_row(place):
        return (place, my_col)

    def in_col(place):
        return (my_row, place)

    def signal_all(sem, place, low, high):
        def one(other, carry):
            pl.semaphore_signal(sem, inc=1, device_id=place(other), device_id_type=MESH)
            return carry

        lax.fori_loop(low, high, one, 0)

    def wait_for(sem, value):
        @pl.when(value > 0)
        def _():
            pl.semaphore_wait(sem, value)

    edge_in = pltpu.make_async_copy(edge_ref, edge_out, edge_sem)
    edge_in.start()

    moves = (
        (my_row + 1, my_col, my_row < n_row - 1, my_row > 0),
        (my_row - 1, my_col, my_row > 0, my_row < n_row - 1),
        (my_row, my_col + 1, my_col < n_col - 1, my_col > 0),
        (my_row, my_col - 1, my_col > 0, my_col < n_col - 1),
    )
    barrier = pltpu.get_barrier_semaphore()
    signal_all(barrier, in_row, my_row + 1, n_row)
    signal_all(barrier, in_col, my_col + 1, n_col)

    with jax.named_scope("early"):
        for copy in early:
            copy.wait()

    part = jnp.sum(node_ref[...].astype(F32).reshape(nodes // 8, 8, width), axis=0)
    pool[my_col, my_row] = jnp.sum(part, axis=0, keepdims=True)
    table[my_col, my_row] = ctx_ref[...]

    def halo_copy(layer, line):
        rows = pl.ds(line * count, count)
        return pltpu.make_async_remote_copy(
            src_ref=picked.at[layer, rows],
            dst_ref=halo.at[layer, rows],
            send_sem=halo_send_sem.at[layer, line],
            recv_sem=halo_recv_sem.at[layer, line],
            device_id=moves[line][:2],
            device_id_type=MESH,
        )

    def halo_start(layer, lines):
        for line in lines:

            @pl.when(moves[line][2])
            def _(line=line):
                halo_copy(layer, line).start()

    def halo_wait(layer):
        for line in range(4):

            @pl.when(moves[line][3])
            def _(line=line):
                halo_copy(layer, line).wait_recv()

    def halo_clear():
        for line in range(4):

            @pl.when(jnp.logical_not(moves[line][3]))
            def _(line=line):
                empty = jnp.zeros((count, width), BF16)
                for layer in range(LAYERS):
                    halo[layer, line * count : (line + 1) * count] = empty

    def halo_sent(layer):
        for line in range(4):

            @pl.when(moves[line][2])
            def _(line=line):
                halo_copy(layer, line).wait_send()

    def row_copies(other):
        return [
            pltpu.make_async_remote_copy(
                src_ref=ref.at[my_col, my_row],
                dst_ref=ref.at[my_col, my_row],
                send_sem=row_send_sem.at[k],
                recv_sem=row_recv_sem.at[k],
                device_id=in_row(other),
                device_id_type=MESH,
            )
            for k, ref in enumerate((table, pool))
        ]

    def col_copies(other):
        return [
            pltpu.make_async_remote_copy(
                src_ref=ref.at[my_col],
                dst_ref=ref.at[my_col],
                send_sem=col_send_sem.at[k],
                recv_sem=col_recv_sem.at[k],
                device_id=in_col(other),
                device_id_type=MESH,
            )
            for k, ref in enumerate((table, pool))
        ]

    def start_all(copies, low, high):
        def one(other, carry):
            for copy in copies(other):
                copy.start()
            return carry

        lax.fori_loop(low, high, one, 0)

    def row_totals():
        held = [ref.at[my_col, pl.ds(0, n_row - 1)] for ref in (table, pool)]
        return [
            pltpu.make_async_remote_copy(
                src_ref=ref,
                dst_ref=ref,
                send_sem=row_send_sem.at[k],
                recv_sem=row_recv_sem.at[k],
                device_id=in_row(lax.rem(my_row + 1, n_row)),
                device_id_type=MESH,
            )
            for k, ref in enumerate(held)
        ]

    def col_totals():
        held = [ref.at[pl.ds(0, n_col - 1)] for ref in (table, pool)]
        return [
            pltpu.make_async_remote_copy(
                src_ref=ref,
                dst_ref=ref,
                send_sem=col_send_sem.at[k],
                recv_sem=col_recv_sem.at[k],
                device_id=in_col(lax.rem(my_col + 1, n_col)),
                device_id_type=MESH,
            )
            for k, ref in enumerate(held)
        ]

    row_known = jnp.minimum(my_row + 2, n_row)

    def near():
        wait_for(near_row_sem, moves[0][2].astype(I32))
        wait_for(near_col_sem, moves[2][2].astype(I32))
        halo_start(0, (0, 2))
        start_all(row_copies, my_row + 1, row_known)

    def first_phase():
        wait_for(ready_row_sem, n_row - 1 - my_row)
        start_all(row_copies, row_known, n_row)

    def second_phase():
        for copy in row_totals():
            copy.wait_recv()
        wait_for(ready_col_sem, n_col - 1 - my_col)
        start_all(col_copies, 0, my_col)
        start_all(col_copies, my_col + 1, n_col)

    ahead = jnp.logical_and(my_row == 0, my_col < 2)

    def between(pair, half):
        if (pair, half) == (1, 0):

            @pl.when(jnp.logical_not(ahead))
            def _():
                near()

        if (pair, half) == (2, 1):

            @pl.when(ahead)
            def _():
                near()

            @pl.when(jnp.logical_not(ahead))
            def _():
                first_phase()

    with jax.named_scope("enter"):
        wait_for(barrier, my_row + my_col)
    start_all(row_copies, 0, my_row)
    signal_all(ready_row_sem, in_row, 0, my_row)

    @pl.when(my_row > 0)
    def _():
        pl.semaphore_signal(near_row_sem, inc=1, device_id=in_row(my_row - 1), device_id_type=MESH)

    @pl.when(my_col > 0)
    def _():
        pl.semaphore_signal(near_col_sem, inc=1, device_id=in_col(my_col - 1), device_id_type=MESH)

    signal_all(ready_col_sem, in_col, 0, my_col)

    for copy in later:
        copy.wait()

    def signed(index, upper):
        return code(index).astype(F32) * jnp.where(upper, -1.0, 1.0)

    sender, receiver = send_ref[...], recv_ref[...]
    in_halo = (sender >= nodes).astype(I32)
    part_size = half_own + (half_halo - half_own) * in_halo
    s_index = sender - nodes * in_halo
    s_upper = s_index >= part_size
    s_index += half_own * in_halo - part_size * s_upper.astype(I32)
    r_upper = receiver >= half_own
    send_row[...] = signed(s_index, s_upper)
    recv_row[...] = signed(receiver - half_own * r_upper.astype(I32), r_upper)

    for line in range(4):
        index = index_ref[line : line + 1, :]
        upper = index >= half_own
        column = as_column(signed(index - half_own * upper.astype(I32), upper))
        rows = slice(line * count, (line + 1) * count)
        index_code[rows, :] = column
        hot_index[rows, :] = pick_rows(jnp.abs(column.astype(BF16)), own_parts)

    def pick(layer, now):
        picked[layer] = take(index_code[...], mm_halves(hot_index[...], fold(now))).astype(BF16)

    pick(0, node_ref)
    halo_start(0, (1, 3))
    with jax.named_scope("rest"):
        for copy in rest:
            copy.wait()
    edge_in.wait()

    def fill_own(layer, now):
        w_pair = jnp.concatenate([ew1[layer, :width], ew1[layer, width : 2 * width]], axis=1)
        both = mm_halves(now[...], w_pair).astype(BF16)
        own_send[...] = jnp.concatenate([both[:half_own, :width], both[half_own:, :width]], axis=1)
        own_recv[...] = jnp.concatenate([both[:half_own, width:], both[half_own:, width:]], axis=1)

    def encode(pair):
        for sub in range(PAIR // LANES):
            line = pair * (PAIR // LANES) + sub
            rows = slice(line * LANES, (line + 1) * LANES)
            recv = recv_row[line : line + 1, :]
            send_code[rows, :] = as_column(send_row[line : line + 1, :])
            recv_code[rows, :] = as_column(recv)

    def gather_phase(layer):
        if layer == 0:
            w_edge = twice(ew1[layer, 2 * width :])
            b_in = eb[0, layer : layer + 1]

        for pair in range(pairs):
            if layer == 0:
                between(pair, 0)
                encode(pair)
            starts = [pair * PAIR + half * BLOCK for half in range(2)]
            blocks = [slice(start, start + BLOCK) for start in starts]
            if layer == 0:
                old = [edge_out[rows, :] for rows in blocks]
                by_edge = mm(jnp.concatenate(old, axis=1), w_edge)
            for half, rows in enumerate(blocks):
                if layer == 0 and half == 1:
                    between(pair, 1)
                send, recv = send_code[rows, :], recv_code[rows, :]
                by_send = mm(pick_rows(jnp.abs(send.astype(BF16)), own_parts), own_send[...])
                by_recv = mm(pick_rows(jnp.abs(recv.astype(BF16)), own_parts), own_recv[...])
                if layer == 0:
                    pre = by_edge[:, half * width : (half + 1) * width] + b_in
                else:
                    pre = pre_ref[rows, :]
                pre += take(send, by_send)
                pre += take(recv, by_recv)
                pre_ref[rows, :] = pre

    def context():
        pooled = jnp.zeros((1, width), F32)
        for col in range(n_col):
            for row in range(n_row):
                pooled += pool[col, row]
        pooled = pooled / math.sqrt(nodes * devices)
        pieces = []
        for _ in range(3):
            pieces.append(pooled.astype(BF16).astype(F32))
            pooled = pooled - pieces[-1]
        pieces = jnp.concatenate(pieces + [jnp.zeros((13, width), F32)], axis=0).astype(BF16)
        w_global = jnp.concatenate([nwg[l] for l in range(LAYERS)], axis=1)
        shift = jnp.sum(mm(pieces, w_global), axis=0, keepdims=True)
        shift += jnp.concatenate([nb[0, l : l + 1] for l in range(LAYERS)], axis=1)
        shared = jnp.concatenate(
            [table[col, row] for row in range(n_row) for col in range(n_col)], axis=0
        )
        w_pair = jnp.concatenate([nw1[l, 2 * width :] for l in range(LAYERS)], axis=1)
        projected = mm(shared, w_pair).astype(BF16)
        ctx_part[...] = mm_halves(hot_region[...], projected) + shift

    fill_own(0, node_ref)
    with jax.named_scope("gather0"):
        gather_phase(0)
    for line in range(nodes // LANES):
        column = as_column(code(region_ref[line : line + 1, :]).astype(F32))
        hot_region[line * LANES : (line + 1) * LANES, :] = pick_rows(
            column.astype(BF16), range(devices * ctx_rows // LANES)
        )
    @pl.when(ahead)
    def _():
        first_phase()

    halo_clear()
    with jax.named_scope("second"):
        second_phase()
    with jax.named_scope("halo0"):
        halo_wait(0)
    fill_halo(at.halo_tab, halo[0], ew1[0, :width])
    edge_phase(at, 0, edge_out, edge_out, ew1)
    node_pre[...] = node_begin(at, 0, node_ref)
    halo_sent(0)
    for copy in row_totals() + col_totals():
        copy.wait_send()
    with jax.named_scope("colwait"):
        for copy in col_totals():
            copy.wait_recv()
    context()
    node_end(at, 0, node_ref, node_pre[...], node_out)
    pick(1, node_out)
    halo_start(1, range(4))
    fill_own(1, node_out)
    with jax.named_scope("gather1"):
        gather_phase(1)
    with jax.named_scope("halo1"):
        halo_wait(1)
    at.halo_last[...] = halo[1]

    with jax.named_scope("sends"):
        halo_sent(1)


HELD = ("ew1", "ew2", "eb", "eg", "nw1", "nw2", "nb", "ng")
CARRIED = ("send_code", "recv_code", "recv_row", "halo_last", "pre_ref", "ctx_part")


def first_entry(n_row, n_col, *refs):
    given, refs = refs[:16], refs[16:]
    outs, refs = refs[: 2 + len(CARRIED) + len(HELD)], refs[2 + len(CARRIED) + len(HELD) :]
    node_out, edge_out = outs[:2]
    at = types.SimpleNamespace(**dict(zip(CARRIED + HELD, outs[2:])))
    at.sums, at.parts, at.y_ref, at.halo_tab, edge_sem, copy_sem = refs[:6]
    node, send, recv, index, ctx, region, nwg = refs[6:13]
    places = [node, None, send, recv, index, ctx, region, at.ew1, at.ew2, at.eb, at.eg]
    places += [at.nw1, nwg, at.nw2, at.nb, at.ng]
    copies = {
        k: pltpu.make_async_copy(given[k], place, copy_sem.at[k])
        for k, place in enumerate(places)
        if place is not None
    }
    groups = (0, 5), (4, 2, 3)
    groups += (tuple(k for k in copies if k not in sum(groups, ())),)
    for k in sum(groups, ()):
        copies[k].start()
    groups = [[copies[k] for k in group] for group in groups]
    places[1] = given[1]
    first_kernel(n_row, n_col, *groups, *places[:8], nwg, edge_sem, at, node_out, edge_out, *refs[13:])


def second_entry(*refs):
    node, edge, refs = refs[0], refs[1], refs[2:]
    count = len(CARRIED) + len(HELD)
    at = types.SimpleNamespace(**dict(zip(CARRIED + HELD, refs[:count])))
    node_out, edge_out, node_new, edge_new, at.sums, at.parts, at.y_ref = refs[count : count + 7]
    at.halo_tab, node_sem, edge_sem = refs[count + 7 :]
    pairs = edge.shape[0] // PAIR

    def edge_copy(pair):
        rows = pl.ds(pair * PAIR, PAIR)
        return pltpu.make_async_copy(edge_new.at[rows], edge_out.at[rows], edge_sem.at[pair])

    fill_halo(at.halo_tab, at.halo_last[...], at.ew1[1, : edge.shape[1]])
    edge_phase(at, 1, edge, edge_new, done=lambda pair: edge_copy(pair).start())
    edge_copy(pairs - 1).start()
    node_end(at, 1, node, node_begin(at, 1, node), node_new)
    node_copy = pltpu.make_async_copy(node_new, node_out, node_sem)
    node_copy.start()
    for pair in range(pairs):
        edge_copy(pair).wait()
    node_copy.wait()


def local(n_row, n_col, *args):
    node, edge, send, recv, index, ctx, region = args[:7]
    nodes, width = node.shape
    edges = edge.shape[0]
    count = index.shape[2]
    devices = n_row * n_col
    half_own, half_halo = nodes // 2, 2 * count
    vmem = pl.BlockSpec(memory_space=pltpu.VMEM)
    hbm = pl.BlockSpec(memory_space=pltpu.HBM)
    dma = pltpu.SemaphoreType.DMA
    operands = (
        node,
        edge,
        send.reshape(edges // LANES, LANES),
        recv.reshape(edges // LANES, LANES),
        index.reshape(4, count),
        ctx,
        region.reshape(nodes // LANES, LANES),
    ) + args[7:]
    operands = tuple(
        jnp.transpose(x, (1, 0, 2)) if x.shape == (LAYERS, 3, width) else x for x in operands
    )
    operands = tuple(pltpu.with_memory_space_constraint(x, pltpu.HBM) for x in operands)
    held = [operands[k] for k in (7, 8, 9, 10, 11, 13, 14, 15)]
    carried = [
        ((edges, width), F32),
        ((edges, width), F32),
        ((edges // LANES, LANES), F32),
        ((4 * count, width), BF16),
        ((edges, width), F32),
        ((nodes, LAYERS * width), F32),
    ]
    shared = [
        jax.ShapeDtypeStruct(node.shape, BF16),
        jax.ShapeDtypeStruct(edge.shape, BF16),
    ]
    passed = shared + [jax.ShapeDtypeStruct(*x) for x in carried]
    passed += [jax.ShapeDtypeStruct(x.shape, x.dtype) for x in held]
    local_scratch = [
        pltpu.VMEM((half_own, 2 * width), F32),
        pltpu.VMEM((PAIR, 2 * width), BF16),
        pltpu.VMEM((2, BLOCK, 2 * width), F32),
        pltpu.VMEM((half_halo, 2 * width), BF16),
    ]
    between = pl.pallas_call(
        functools.partial(first_entry, n_row, n_col),
        out_shape=tuple(passed),
        in_specs=[hbm] * len(operands),
        out_specs=(vmem,) * len(passed),
        scratch_shapes=local_scratch
        + [dma(()), dma((len(operands),))]
        + [pltpu.VMEM(operands[k].shape, operands[k].dtype) for k in (0, 2, 3, 4, 5, 6, 12)]
        + [
            pltpu.VMEM((edges // LANES, LANES), F32),
            pltpu.VMEM((4 * count, half_own), BF16),
            pltpu.VMEM((nodes, devices * ctx.shape[0]), BF16),
            pltpu.VMEM((4 * count, width), F32),
            pltpu.VMEM((LAYERS, 4 * count, width), BF16),
            pltpu.VMEM((LAYERS, 4 * count, width), BF16),
            pltpu.VMEM((n_col, n_row, ctx.shape[0], width), BF16),
            pltpu.VMEM((n_col, n_row, 1, width), F32),
            pltpu.VMEM((nodes, width), F32),
            pltpu.VMEM((half_own, 2 * width), BF16),
            pltpu.VMEM((half_own, 2 * width), BF16),
            dma((LAYERS, 4)),
            dma((LAYERS, 4)),
            dma((2,)),
            dma((2,)),
            dma((2,)),
            dma((2,)),
            pltpu.SemaphoreType.REGULAR,
            pltpu.SemaphoreType.REGULAR,
            pltpu.SemaphoreType.REGULAR,
            pltpu.SemaphoreType.REGULAR,
        ],
        compiler_params=pltpu.CompilerParams(
            collective_id=0, has_side_effects=True, vmem_limit_bytes=24 * 1024 * 1024
        ),
        name="mesh_first",
    )(*operands)
    return pl.pallas_call(
        second_entry,
        out_shape=tuple(shared),
        in_specs=[vmem] * len(passed),
        out_specs=(hbm, hbm),
        scratch_shapes=[pltpu.VMEM(node.shape, BF16), pltpu.VMEM(edge.shape, BF16)]
        + local_scratch
        + [dma(()), dma((edges // PAIR,))],
        compiler_params=pltpu.CompilerParams(vmem_limit_bytes=24 * 1024 * 1024),
        name="mesh_second",
    )(*between)


def solution(mesh):
    both = ("row", "col")
    split = (P(both, None), P(both, None), P(both), P(both), P(both, None, None), P(both, None), P(both))
    return jax.shard_map(
        functools.partial(local, mesh.shape["row"], mesh.shape["col"]),
        mesh=mesh,
        in_specs=split + (P(),) * 9,
        out_specs=(P(both, None), P(both, None)),
        check_vma=False,
    )
```

```python
import functools
import math
import types

import jax
import jax.numpy as jnp
from jax import lax
from jax.experimental import pallas as pl
from jax.experimental.pallas import tpu as pltpu
from jax.sharding import PartitionSpec as P

LAYERS = 2
EPS = 1e-05
LANES = 128
BLOCK = 512
PAIR = 2 * BLOCK
STEP = 2048
F32 = jnp.float32
BF16 = jnp.bfloat16
I32 = jnp.int32
MESH = pl.DeviceIdType.MESH


def mm(a, b):
    return jnp.dot(a, b, preferred_element_type=F32)


def mm_halves(a, b):
    half = a.shape[0] // 2
    return jnp.concatenate([mm(a[:half], b), mm(a[half:], b)], axis=0)


def iota(axis):
    return lax.broadcasted_iota(I32, (LANES, LANES), axis)


def as_column(row):
    return jnp.transpose(jnp.broadcast_to(row, (LANES, LANES)))


def code(index):
    return (LANES + (index & (LANES - 1))) << (index >> 7)


def pick_parts(coded, axis, parts):
    base = (iota(axis) + LANES).astype(F32)
    one, zero = jnp.ones((), BF16), jnp.zeros((), BF16)
    if axis == 0:
        base = base.astype(BF16)
        masks = [coded * jnp.asarray(0.5**part, BF16) == base for part in parts]
    else:
        masks = [coded == (base * float(1 << part)).astype(BF16) for part in parts]
    return [jnp.where(mask, one, zero) for mask in masks]


def pick_rows(coded, parts):
    blocks = []
    for start in range(0, coded.shape[0], LANES):
        blocks.append(jnp.concatenate(pick_parts(coded[start : start + LANES], 1, parts), axis=1))
    return blocks[0] if len(blocks) == 1 else jnp.concatenate(blocks, axis=0)


def centre(values):
    values = values.astype(F32)
    return values - jnp.mean(values, axis=-1, keepdims=True)


def twice(weight):
    zero = jnp.zeros_like(weight)
    top = jnp.concatenate([weight, zero], axis=1)
    return jnp.concatenate([top, jnp.concatenate([zero, weight], axis=1)], axis=0)


def norm(centred, gain, shift):
    width = centred.shape[-1]
    total = jnp.sum(centred * centred, axis=-1, keepdims=True)
    return centred * lax.rsqrt(total + width * EPS) * (gain * math.sqrt(width)) + shift


def fold(ref):
    half = ref.shape[0] // 2
    return jnp.concatenate([ref[:half, :], ref[half:, :]], axis=1)


def take(coded, both):
    width = both.shape[1] // 2
    return jnp.where(coded < 0, both[:, width:], both[:, :width])


def scatter(at, pair):
    own_parts = range(at.sums.shape[0] // LANES)
    blocks = []
    for line in range(pair * STEP // LANES, (pair + 1) * STEP // LANES):
        coded = jnp.broadcast_to(jnp.abs(at.recv_row[line : line + 1, :]), (LANES, LANES))
        blocks.append(jnp.concatenate(pick_parts(coded.astype(BF16), 0, own_parts), axis=0))
    term = mm_halves(jnp.concatenate(blocks, axis=1), at.parts[...])
    if pair == 0:
        at.sums[...] = term
    else:
        at.sums[...] += term


def edge_phase(at, layer, old_ref, new_ref, ew1=None, done=None):
    edges, width = old_ref.shape
    half_own, half_halo = at.sums.shape[0], at.halo_tab.shape[0]
    pairs = edges // STEP
    halo_parts = range(half_own // LANES, (half_own + half_halo) // LANES)
    w_out = twice(centre(at.ew2[layer]).astype(BF16))
    b_out = centre(at.eb[1, layer : layer + 1])
    if ew1 is not None:
        w_next = twice(ew1[layer + 1, 2 * width :])

    def blocks_of(pair):
        starts = [pair * STEP + half * STEP // 2 for half in range(2)]
        return [slice(start, start + STEP // 2) for start in starts]

    def columns(half):
        return slice(half * width, (half + 1) * width)

    def begin(pair):
        hidden = []
        for rows in blocks_of(pair):
            send = at.send_code[rows, :]
            hot = pick_rows(jnp.abs(send.astype(BF16)), halo_parts)
            pre = at.pre_ref[rows, :] + take(send, mm(hot, at.halo_tab[...]))
            hidden.append(jnp.maximum(pre.astype(BF16), jnp.zeros((), BF16)))
        at.y_ref[pair % 2] = mm_halves(jnp.concatenate(hidden, axis=1), w_out)

    def finish(pair):
        for half, rows in enumerate(blocks_of(pair)):
            centred = at.y_ref[pair % 2, :, columns(half)] + b_out
            new = old_ref[rows, :].astype(F32)
            new += norm(centred, at.eg[layer : layer + 1], at.eb[2, layer : layer + 1])
            new = new.astype(BF16)
            new_ref[rows, :] = new
            upper = at.recv_code[rows, :].astype(BF16) < 0
            held = slice(half * STEP // 2, (half + 1) * STEP // 2)
            zero = jnp.zeros((), BF16)
            at.parts[held, :width] = jnp.where(upper, zero, new)
            at.parts[held, width:] = jnp.where(upper, new, zero)

    def carry_on(pair):
        if ew1 is not None:
            news = [new_ref[rows, :] for rows in blocks_of(pair)]
            by_edge = mm(jnp.concatenate(news, axis=1), w_next)
            for half, rows in enumerate(blocks_of(pair)):
                at.pre_ref[rows, :] = by_edge[:, columns(half)] + at.eb[0, layer + 1 : layer + 2]

    for step in range(pairs + 1):
        if step < pairs:
            begin(step)
        if step > 1:
            scatter(at, step - 2)
            carry_on(step - 2)
        if step > 0:
            finish(step - 1)
        if done is not None and step > 1:
            done(step - 2)
    carry_on(pairs - 1)


def fill_halo(halo_tab, halo, weight):
    rows = mm_halves(halo, weight).astype(BF16)
    half = rows.shape[0] // 2
    halo_tab[...] = jnp.concatenate([rows[:half], rows[half:]], axis=1)


def node_begin(at, layer, now):
    width = now.shape[1]
    scatter(at, at.recv_row.shape[0] * LANES // STEP - 1)
    summed = jnp.concatenate([at.sums[:, :width], at.sums[:, width:]], axis=0).astype(BF16)
    feats = jnp.concatenate([now[...], summed], axis=1)
    return mm_halves(feats, at.nw1[layer, : 2 * width])


def node_end(at, layer, now, pre, new_ref):
    width = now.shape[1]
    pre += at.ctx_part[:, layer * width : (layer + 1) * width]
    hidden = jnp.maximum(pre, 0.0).astype(BF16)
    w_out, b_out = centre(at.nw2[layer]).astype(BF16), centre(at.nb[1, layer : layer + 1])
    new = now[...].astype(F32)
    new += norm(mm_halves(hidden, w_out) + b_out, at.ng[layer : layer + 1], at.nb[2, layer : layer + 1])
    new_ref[...] = new.astype(BF16)


def first_kernel(
    n_row,
    n_col,
    early,
    later,
    rest,
    node_ref,
    edge_ref,
    send_ref,
    recv_ref,
    index_ref,
    ctx_ref,
    region_ref,
    ew1,
    nwg,
    edge_sem,
    at,
    node_out,
    edge_out,
    send_row,
    hot_index,
    hot_region,
    index_code,
    picked,
    halo,
    table,
    pool,
    node_pre,
    own_send,
    own_recv,
    halo_send_sem,
    halo_recv_sem,
    row_send_sem,
    row_recv_sem,
    col_send_sem,
    col_recv_sem,
    near_row_sem,
    near_col_sem,
    ready_row_sem,
    ready_col_sem,
):
    my_row, my_col = lax.axis_index("row"), lax.axis_index("col")
    send_code, recv_code, recv_row = at.send_code, at.recv_code, at.recv_row
    pre_ref, ctx_part = at.pre_ref, at.ctx_part
    eb, nw1, nb = at.eb, at.nw1, at.nb
    devices = n_row * n_col
    nodes, width = node_ref.shape
    edges = edge_ref.shape[0]
    count = index_ref.shape[1]
    half_own, half_halo = nodes // 2, 2 * count
    own_parts = range(half_own // LANES)
    ctx_rows = ctx_ref.shape[0]
    pairs = edges // PAIR

    def in_row(place):
        return (place, my_col)

    def in_col(place):
        return (my_row, place)

    def signal_all(sem, place, low, high):
        def one(other, carry):
            pl.semaphore_signal(sem, inc=1, device_id=place(other), device_id_type=MESH)
            return carry

        lax.fori_loop(low, high, one, 0)

    def wait_for(sem, value):
        @pl.when(value > 0)
        def _():
            pl.semaphore_wait(sem, value)

    edge_in = pltpu.make_async_copy(edge_ref, edge_out, edge_sem)
    edge_in.start()

    moves = (
        (my_row + 1, my_col, my_row < n_row - 1, my_row > 0),
        (my_row - 1, my_col, my_row > 0, my_row < n_row - 1),
        (my_row, my_col + 1, my_col < n_col - 1, my_col > 0),
        (my_row, my_col - 1, my_col > 0, my_col < n_col - 1),
    )
    barrier = pltpu.get_barrier_semaphore()
    signal_all(barrier, in_row, my_row + 1, n_row)
    signal_all(barrier, in_col, my_col + 1, n_col)

    with jax.named_scope("early"):
        for copy in early:
            copy.wait()

    part = jnp.sum(node_ref[...].astype(F32).reshape(nodes // 8, 8, width), axis=0)
    pool[my_col, my_row] = jnp.sum(part, axis=0, keepdims=True)
    table[my_col, my_row] = ctx_ref[...]

    def halo_copy(layer, line):
        rows = pl.ds(line * count, count)
        return pltpu.make_async_remote_copy(
            src_ref=picked.at[layer, rows],
            dst_ref=halo.at[layer, rows],
            send_sem=halo_send_sem.at[layer, line],
            recv_sem=halo_recv_sem.at[layer, line],
            device_id=moves[line][:2],
            device_id_type=MESH,
        )

    def halo_start(layer, lines):
        for line in lines:

            @pl.when(moves[line][2])
            def _(line=line):
                halo_copy(layer, line).start()

    def halo_wait(layer):
        for line in range(4):

            @pl.when(moves[line][3])
            def _(line=line):
                halo_copy(layer, line).wait_recv()

    def halo_clear():
        for line in range(4):

            @pl.when(jnp.logical_not(moves[line][3]))
            def _(line=line):
                empty = jnp.zeros((count, width), BF16)
                for layer in range(LAYERS):
                    halo[layer, line * count : (line + 1) * count] = empty

    def halo_sent(layer):
        for line in range(4):

            @pl.when(moves[line][2])
            def _(line=line):
                halo_copy(layer, line).wait_send()

    def row_copies(other):
        return [
            pltpu.make_async_remote_copy(
                src_ref=ref.at[my_col, my_row],
                dst_ref=ref.at[my_col, my_row],
                send_sem=row_send_sem.at[k],
                recv_sem=row_recv_sem.at[k],
                device_id=in_row(other),
                device_id_type=MESH,
            )
            for k, ref in enumerate((table, pool))
        ]

    def col_copies(other):
        return [
            pltpu.make_async_remote_copy(
                src_ref=ref.at[my_col],
                dst_ref=ref.at[my_col],
                send_sem=col_send_sem.at[k],
                recv_sem=col_recv_sem.at[k],
                device_id=in_col(other),
                device_id_type=MESH,
            )
            for k, ref in enumerate((table, pool))
        ]

    def start_all(copies, low, high):
        def one(other, carry):
            for copy in copies(other):
                copy.start()
            return carry

        lax.fori_loop(low, high, one, 0)

    def row_totals():
        held = [ref.at[my_col, pl.ds(0, n_row - 1)] for ref in (table, pool)]
        return [
            pltpu.make_async_remote_copy(
                src_ref=ref,
                dst_ref=ref,
                send_sem=row_send_sem.at[k],
                recv_sem=row_recv_sem.at[k],
                device_id=in_row(lax.rem(my_row + 1, n_row)),
                device_id_type=MESH,
            )
            for k, ref in enumerate(held)
        ]

    def col_totals():
        held = [ref.at[pl.ds(0, n_col - 1)] for ref in (table, pool)]
        return [
            pltpu.make_async_remote_copy(
                src_ref=ref,
                dst_ref=ref,
                send_sem=col_send_sem.at[k],
                recv_sem=col_recv_sem.at[k],
                device_id=in_col(lax.rem(my_col + 1, n_col)),
                device_id_type=MESH,
            )
            for k, ref in enumerate(held)
        ]

    row_known = jnp.minimum(my_row + 2, n_row)

    def near():
        wait_for(near_row_sem, moves[0][2].astype(I32))
        wait_for(near_col_sem, moves[2][2].astype(I32))
        halo_start(0, (0, 2))
        start_all(row_copies, my_row + 1, row_known)

    def first_phase():
        wait_for(ready_row_sem, n_row - 1 - my_row)
        start_all(row_copies, row_known, n_row)

    def second_phase():
        for copy in row_totals():
            copy.wait_recv()
        wait_for(ready_col_sem, n_col - 1 - my_col)
        start_all(col_copies, 0, my_col)
        start_all(col_copies, my_col + 1, n_col)

    ahead = jnp.logical_and(my_row == 0, my_col < 2)

    def between(pair, half):
        if (pair, half) == (1, 0):

            @pl.when(jnp.logical_not(ahead))
            def _():
                near()

        if (pair, half) == (2, 1):

            @pl.when(ahead)
            def _():
                near()

            @pl.when(jnp.logical_not(ahead))
            def _():
                first_phase()

    with jax.named_scope("enter"):
        wait_for(barrier, my_row + my_col)
    start_all(row_copies, 0, my_row)
    signal_all(ready_row_sem, in_row, 0, my_row)

    @pl.when(my_row > 0)
    def _():
        pl.semaphore_signal(near_row_sem, inc=1, device_id=in_row(my_row - 1), device_id_type=MESH)

    @pl.when(my_col > 0)
    def _():
        pl.semaphore_signal(near_col_sem, inc=1, device_id=in_col(my_col - 1), device_id_type=MESH)

    signal_all(ready_col_sem, in_col, 0, my_col)

    for copy in later:
        copy.wait()

    def signed(index, upper):
        return code(index).astype(F32) * jnp.where(upper, -1.0, 1.0)

    sender, receiver = send_ref[...], recv_ref[...]
    in_halo = (sender >= nodes).astype(I32)
    part_size = half_own + (half_halo - half_own) * in_halo
    s_index = sender - nodes * in_halo
    s_upper = s_index >= part_size
    s_index += half_own * in_halo - part_size * s_upper.astype(I32)
    r_upper = receiver >= half_own
    send_row[...] = signed(s_index, s_upper)
    recv_row[...] = signed(receiver - half_own * r_upper.astype(I32), r_upper)

    for line in range(4):
        index = index_ref[line : line + 1, :]
        upper = index >= half_own
        column = as_column(signed(index - half_own * upper.astype(I32), upper))
        rows = slice(line * count, (line + 1) * count)
        index_code[rows, :] = column
        hot_index[rows, :] = pick_rows(jnp.abs(column.astype(BF16)), own_parts)

    def pick(layer, now):
        picked[layer] = take(index_code[...], mm_halves(hot_index[...], fold(now))).astype(BF16)

    pick(0, node_ref)
    halo_start(0, (1, 3))
    with jax.named_scope("rest"):
        for copy in rest:
            copy.wait()
    edge_in.wait()

    def fill_own(layer, now):
        w_pair = jnp.concatenate([ew1[layer, :width], ew1[layer, width : 2 * width]], axis=1)
        both = mm_halves(now[...], w_pair).astype(BF16)
        own_send[...] = jnp.concatenate([both[:half_own, :width], both[half_own:, :width]], axis=1)
        own_recv[...] = jnp.concatenate([both[:half_own, width:], both[half_own:, width:]], axis=1)

    def encode(pair):
        for sub in range(PAIR // LANES):
            line = pair * (PAIR // LANES) + sub
            rows = slice(line * LANES, (line + 1) * LANES)
            recv = recv_row[line : line + 1, :]
            send_code[rows, :] = as_column(send_row[line : line + 1, :])
            recv_code[rows, :] = as_column(recv)

    def gather_phase(layer):
        if layer == 0:
            w_edge = twice(ew1[layer, 2 * width :])
            b_in = eb[0, layer : layer + 1]

        for pair in range(pairs):
            if layer == 0:
                between(pair, 0)
                encode(pair)
            starts = [pair * PAIR + half * BLOCK for half in range(2)]
            blocks = [slice(start, start + BLOCK) for start in starts]
            if layer == 0:
                old = [edge_out[rows, :] for rows in blocks]
                by_edge = mm(jnp.concatenate(old, axis=1), w_edge)
            for half, rows in enumerate(blocks):
                if layer == 0 and half == 1:
                    between(pair, 1)
                send, recv = send_code[rows, :], recv_code[rows, :]
                by_send = mm(pick_rows(jnp.abs(send.astype(BF16)), own_parts), own_send[...])
                by_recv = mm(pick_rows(jnp.abs(recv.astype(BF16)), own_parts), own_recv[...])
                if layer == 0:
                    pre = by_edge[:, half * width : (half + 1) * width] + b_in
                else:
                    pre = pre_ref[rows, :]
                pre += take(send, by_send)
                pre += take(recv, by_recv)
                pre_ref[rows, :] = pre

    def context():
        pooled = jnp.zeros((1, width), F32)
        for col in range(n_col):
            for row in range(n_row):
                pooled += pool[col, row]
        pooled = pooled / math.sqrt(nodes * devices)
        pieces = []
        for _ in range(3):
            pieces.append(pooled.astype(BF16).astype(F32))
            pooled = pooled - pieces[-1]
        pieces = jnp.concatenate(pieces + [jnp.zeros((13, width), F32)], axis=0).astype(BF16)
        w_global = jnp.concatenate([nwg[l] for l in range(LAYERS)], axis=1)
        shift = jnp.sum(mm(pieces, w_global), axis=0, keepdims=True)
        shift += jnp.concatenate([nb[0, l : l + 1] for l in range(LAYERS)], axis=1)
        shared = jnp.concatenate(
            [table[col, row] for row in range(n_row) for col in range(n_col)], axis=0
        )
        w_pair = jnp.concatenate([nw1[l, 2 * width :] for l in range(LAYERS)], axis=1)
        projected = mm(shared, w_pair).astype(BF16)
        ctx_part[...] = mm_halves(hot_region[...], projected) + shift

    fill_own(0, node_ref)
    with jax.named_scope("gather0"):
        gather_phase(0)
    for line in range(nodes // LANES):
        column = as_column(code(region_ref[line : line + 1, :]).astype(F32))
        hot_region[line * LANES : (line + 1) * LANES, :] = pick_rows(
            column.astype(BF16), range(devices * ctx_rows // LANES)
        )
    @pl.when(ahead)
    def _():
        first_phase()

    halo_clear()
    with jax.named_scope("second"):
        second_phase()
    with jax.named_scope("halo0"):
        halo_wait(0)
    fill_halo(at.halo_tab, halo[0], ew1[0, :width])
    edge_phase(at, 0, edge_out, edge_out, ew1)
    node_pre[...] = node_begin(at, 0, node_ref)
    halo_sent(0)
    for copy in row_totals() + col_totals():
        copy.wait_send()
    with jax.named_scope("colwait"):
        for copy in col_totals():
            copy.wait_recv()
    context()
    node_end(at, 0, node_ref, node_pre[...], node_out)
    pick(1, node_out)
    halo_start(1, range(4))
    fill_own(1, node_out)
    with jax.named_scope("gather1"):
        gather_phase(1)
    with jax.named_scope("halo1"):
        halo_wait(1)
    at.halo_last[...] = halo[1]

    with jax.named_scope("sends"):
        halo_sent(1)


HELD = ("ew1", "ew2", "eb", "eg", "nw1", "nw2", "nb", "ng")
CARRIED = ("send_code", "recv_code", "recv_row", "halo_last", "pre_ref", "ctx_part")


def first_entry(n_row, n_col, *refs):
    given, refs = refs[:16], refs[16:]
    outs, refs = refs[: 2 + len(CARRIED) + len(HELD)], refs[2 + len(CARRIED) + len(HELD) :]
    node_out, edge_out = outs[:2]
    at = types.SimpleNamespace(**dict(zip(CARRIED + HELD, outs[2:])))
    at.sums, at.parts, at.y_ref, at.halo_tab, edge_sem, copy_sem = refs[:6]
    node, send, recv, index, ctx, region, nwg = refs[6:13]
    places = [node, None, send, recv, index, ctx, region, at.ew1, at.ew2, at.eb, at.eg]
    places += [at.nw1, nwg, at.nw2, at.nb, at.ng]
    copies = {
        k: pltpu.make_async_copy(given[k], place, copy_sem.at[k])
        for k, place in enumerate(places)
        if place is not None
    }
    groups = (0, 5), (4, 2, 3)
    groups += (tuple(k for k in copies if k not in sum(groups, ())),)
    for k in sum(groups, ()):
        copies[k].start()
    groups = [[copies[k] for k in group] for group in groups]
    places[1] = given[1]
    first_kernel(n_row, n_col, *groups, *places[:8], nwg, edge_sem, at, node_out, edge_out, *refs[13:])


def second_entry(*refs):
    node, edge, refs = refs[0], refs[1], refs[2:]
    count = len(CARRIED) + len(HELD)
    at = types.SimpleNamespace(**dict(zip(CARRIED + HELD, refs[:count])))
    node_out, edge_out, node_new, edge_new, at.sums, at.parts, at.y_ref = refs[count : count + 7]
    at.halo_tab, node_sem, edge_sem = refs[count + 7 :]
    pairs = edge.shape[0] // STEP

    def edge_copy(pair):
        rows = pl.ds(pair * STEP, STEP)
        return pltpu.make_async_copy(edge_new.at[rows], edge_out.at[rows], edge_sem.at[pair])

    fill_halo(at.halo_tab, at.halo_last[...], at.ew1[1, : edge.shape[1]])
    edge_phase(at, 1, edge, edge_new, done=lambda pair: edge_copy(pair).start())
    edge_copy(pairs - 1).start()
    node_end(at, 1, node, node_begin(at, 1, node), node_new)
    node_copy = pltpu.make_async_copy(node_new, node_out, node_sem)
    node_copy.start()
    for pair in range(pairs):
        edge_copy(pair).wait()
    node_copy.wait()


def local(n_row, n_col, *args):
    node, edge, send, recv, index, ctx, region = args[:7]
    nodes, width = node.shape
    edges = edge.shape[0]
    count = index.shape[2]
    devices = n_row * n_col
    half_own, half_halo = nodes // 2, 2 * count
    vmem = pl.BlockSpec(memory_space=pltpu.VMEM)
    hbm = pl.BlockSpec(memory_space=pltpu.HBM)
    dma = pltpu.SemaphoreType.DMA
    operands = (
        node,
        edge,
        send.reshape(edges // LANES, LANES),
        recv.reshape(edges // LANES, LANES),
        index.reshape(4, count),
        ctx,
        region.reshape(nodes // LANES, LANES),
    ) + args[7:]
    operands = tuple(
        jnp.transpose(x, (1, 0, 2)) if x.shape == (LAYERS, 3, width) else x for x in operands
    )
    operands = tuple(pltpu.with_memory_space_constraint(x, pltpu.HBM) for x in operands)
    held = [operands[k] for k in (7, 8, 9, 10, 11, 13, 14, 15)]
    carried = [
        ((edges, width), F32),
        ((edges, width), F32),
        ((edges // LANES, LANES), F32),
        ((4 * count, width), BF16),
        ((edges, width), F32),
        ((nodes, LAYERS * width), F32),
    ]
    shared = [
        jax.ShapeDtypeStruct(node.shape, BF16),
        jax.ShapeDtypeStruct(edge.shape, BF16),
    ]
    passed = shared + [jax.ShapeDtypeStruct(*x) for x in carried]
    passed += [jax.ShapeDtypeStruct(x.shape, x.dtype) for x in held]
    local_scratch = [
        pltpu.VMEM((half_own, 2 * width), F32),
        pltpu.VMEM((STEP, 2 * width), BF16),
        pltpu.VMEM((2, STEP // 2, 2 * width), F32),
        pltpu.VMEM((half_halo, 2 * width), BF16),
    ]
    between = pl.pallas_call(
        functools.partial(first_entry, n_row, n_col),
        out_shape=tuple(passed),
        in_specs=[hbm] * len(operands),
        out_specs=(vmem,) * len(passed),
        scratch_shapes=local_scratch
        + [dma(()), dma((len(operands),))]
        + [pltpu.VMEM(operands[k].shape, operands[k].dtype) for k in (0, 2, 3, 4, 5, 6, 12)]
        + [
            pltpu.VMEM((edges // LANES, LANES), F32),
            pltpu.VMEM((4 * count, half_own), BF16),
            pltpu.VMEM((nodes, devices * ctx.shape[0]), BF16),
            pltpu.VMEM((4 * count, width), F32),
            pltpu.VMEM((LAYERS, 4 * count, width), BF16),
            pltpu.VMEM((LAYERS, 4 * count, width), BF16),
            pltpu.VMEM((n_col, n_row, ctx.shape[0], width), BF16),
            pltpu.VMEM((n_col, n_row, 1, width), F32),
            pltpu.VMEM((nodes, width), F32),
            pltpu.VMEM((half_own, 2 * width), BF16),
            pltpu.VMEM((half_own, 2 * width), BF16),
            dma((LAYERS, 4)),
            dma((LAYERS, 4)),
            dma((2,)),
            dma((2,)),
            dma((2,)),
            dma((2,)),
            pltpu.SemaphoreType.REGULAR,
            pltpu.SemaphoreType.REGULAR,
            pltpu.SemaphoreType.REGULAR,
            pltpu.SemaphoreType.REGULAR,
        ],
        compiler_params=pltpu.CompilerParams(
            collective_id=0, has_side_effects=True, vmem_limit_bytes=24 * 1024 * 1024
        ),
        name="mesh_first",
    )(*operands)
    return pl.pallas_call(
        second_entry,
        out_shape=tuple(shared),
        in_specs=[vmem] * len(passed),
        out_specs=(hbm, hbm),
        scratch_shapes=[pltpu.VMEM(node.shape, BF16), pltpu.VMEM(edge.shape, BF16)]
        + local_scratch
        + [dma(()), dma((edges // STEP,))],
        compiler_params=pltpu.CompilerParams(vmem_limit_bytes=24 * 1024 * 1024),
        name="mesh_second",
    )(*between)


def solution(mesh):
    both = ("row", "col")
    split = (P(both, None), P(both, None), P(both), P(both), P(both, None, None), P(both, None), P(both))
    return jax.shard_map(
        functools.partial(local, mesh.shape["row"], mesh.shape["col"]),
        mesh=mesh,
        in_specs=split + (P(),) * 9,
        out_specs=(P(both, None), P(both, None)),
        check_vma=False,
    )
```
